128 devices in a mesh: grp: 4 (over x_lo, core), dev: 32 (over z, x_hi, y).
Axes of the slice: x: 4 (x_hi: 2, x_lo: 2; x = x_hi * 2 + x_lo), y: 4, z: 4, core: 2. Of those that a mesh axis runs over, the one named last changes fastest.
Arguments:
- student: bfloat16 [16384, 1024], P(('grp', 'dev')), may hold values from -0.19921875 to 0.19921875
- teacher: bfloat16 [16384, 1024], P(('grp', 'dev')), may hold values from -0.19921875 to 0.19921875
- labels: int32 [16384], P(('grp', 'dev')), may hold values from 0 to 999, as said below
Outputs:
- supcon_loss: float32 [], replicated
- relation_loss: float32 [], replicated
- feature_grad: float32 [16384, 1024], P(('grp', 'dev'))
The draws below stay inside these ranges and needn't reach their ends.
Inputs may be any that keep to these rules, and one draw needn't show every extreme that they name: `labels`: each label from 875 upward belongs to exactly one view of the batch; every other view has a label below 875.
All inputs are finite; a program needn't handle non-finite values.
Results may differ from the reference program's by a relative error of at most 0.0003.
The reference program's roundings to bfloat16 on the way count: a program that leaves them out, or rounds other values in their place, can miss the bound.
Values may be sent and summed in bfloat16 or wider, within the bound.
A program may use at most 128 MiB of HBM per device.

```python
import math
import jax
import jax.numpy as jnp
from jax import lax

D = 1024
CLASSES = 1000
VIEWS = 16384


def draw_labels(key, part):
    reserved = CLASSES // 8
    common_key = jax.random.fold_in(key, 11)
    place_key = jax.random.fold_in(key, 23)
    common = jax.random.randint(common_key, (VIEWS,), 0, CLASSES - reserved, dtype=jnp.int32)
    chosen = jax.random.permutation(place_key, VIEWS)[:reserved].astype(jnp.int32)
    single = CLASSES - reserved + jnp.arange(reserved, dtype=jnp.int32)
    return common.at[chosen].set(single)


def levels(key, dims, cuts, low, high):
    loudness, own = 1.0, jax.random.fold_in(key, 6)
    for position, shards_of in cuts:
        steps = jnp.exp(jax.random.uniform(jax.random.fold_in(own, position), (shards_of,), jnp.float32, low / len(cuts), high / len(cuts)))
        loudness = loudness * jnp.repeat(steps, dims[position] // shards_of).reshape([-1 if axis == position else 1 for axis in range(len(dims))])
    return loudness


def bell_draw(stream_key, extent, scale, limit, shards=(), kind=jnp.bfloat16):
    result = scale * jax.random.normal(stream_key, extent, jnp.float32)
    if shards:
        result = result * levels(stream_key, extent, shards, -0.22, 0.18)
    return jnp.clip(result, -limit, limit).astype(kind)


def setup_inputs(seed: int = 0) -> dict:
    arg_keys = jax.random.split(jax.random.key(seed), 4)
    return {
        "student": bell_draw(arg_keys[0], (VIEWS, D), 0.03125, 0.19921875, ((0, 128),)),
        "teacher": bell_draw(arg_keys[1], (VIEWS, D), 0.03125, 0.19921875, ((0, 128),)),
        "labels": draw_labels(jax.random.fold_in(arg_keys[3], 71), 0),
    }


temp_sup = 0.1
temp_student = 0.2
temp_teacher = 0.05
epsilon = 1e-06

def unit_rows(raw):
    values = raw.astype(jnp.float32)
    scaling = lax.rsqrt(lax.optimization_barrier(jnp.sum(values * values, axis=1, keepdims=True)) + epsilon)
    return (values * scaling, scaling)

def inner_rows(left, right):
    return lax.dot_general(left, right, (((1,), (1,)), ((), ())), preferred_element_type=jnp.float32)

def tile_terms(anchor_unit, anchor_teacher, anchor_label, anchor_place, key_unit, key_teacher, key_label, key_place):
    similar = inner_rows(anchor_unit, key_unit)
    teacher_sim = inner_rows(anchor_teacher, key_teacher)
    distinct = anchor_place[:, None] != key_place[None, :]
    positive = jnp.logical_and(anchor_label[:, None] == key_label[None, :], distinct).astype(jnp.float32)
    empty = jnp.zeros_like(similar)
    sup_exp = jnp.where(distinct, jnp.exp((similar - 1.0) / temp_sup), empty)
    rel_exp = jnp.where(distinct, jnp.exp((similar - 1.0) / temp_student), empty)
    teacher_exp = jnp.where(distinct, jnp.exp((teacher_sim - 1.0) / temp_teacher), empty)
    return (similar, positive, sup_exp, rel_exp, teacher_exp)

def tile_stats(terms):
    similar, positive, sup_exp, rel_exp, teacher_exp = terms
    return (lax.optimization_barrier(jnp.sum(sup_exp, axis=1)), lax.optimization_barrier(jnp.sum(rel_exp, axis=1)), lax.optimization_barrier(jnp.sum(teacher_exp, axis=1)), lax.optimization_barrier(jnp.sum(teacher_exp * similar, axis=1)), lax.optimization_barrier(jnp.sum(positive * similar, axis=1)), lax.optimization_barrier(jnp.sum(positive, axis=1)))

def coefficient(terms, sup_total, rel_total, teacher_total, positives):
    similar, positive, sup_exp, rel_exp, teacher_exp = terms
    return (sup_exp / sup_total - positive / positives) / temp_sup + (rel_exp / rel_total - teacher_exp / teacher_total) / temp_student

def row_losses(stats):
    sup_total, rel_total, teacher_total, teacher_mix, positive_sum, positive_count = stats
    positives = jnp.maximum(positive_count, 1.0)
    contrast = (1.0 - positive_sum / positives) / temp_sup + jnp.log(sup_total)
    relation = (1.0 - teacher_mix / teacher_total) / temp_student + jnp.log(rel_total)
    return (contrast, relation)

def reference(student, teacher, labels):
    view_count, width = student.shape
    unit_student, scaling = unit_rows(student)
    unit_rounded = unit_student.astype(jnp.bfloat16)
    teacher_rounded = unit_rows(teacher)[0].astype(jnp.bfloat16)
    places = jnp.arange(view_count, dtype=jnp.int32)
    block_rows = math.gcd(view_count, 512)
    block_total = view_count // block_rows
    blocked = (unit_rounded.reshape(block_total, block_rows, width), teacher_rounded.reshape(block_total, block_rows, width), labels.reshape(block_total, block_rows), places.reshape(block_total, block_rows))

    def stats_block(operands):
        return tile_stats(tile_terms(operands[0], operands[1], operands[2], operands[3], unit_rounded, teacher_rounded, labels, places))
    stats = lax.map(stats_block, blocked)
    stats = tuple((item.reshape(view_count) for item in stats))
    contrast, relation = row_losses(stats)
    coef_stats = (stats[0], stats[1], stats[2], jnp.maximum(stats[5], 1.0))
    blocked_stats = tuple((item.reshape(block_total, block_rows) for item in coef_stats))

    def grad_step(key_sum, operands):
        terms = tile_terms(operands[0], operands[1], operands[2], operands[3], unit_rounded, teacher_rounded, labels, places)
        coef = coefficient(terms, operands[4][:, None], operands[5][:, None], operands[6][:, None], operands[7][:, None]).astype(jnp.bfloat16)
        anchor_part = jnp.dot(coef, unit_rounded, preferred_element_type=jnp.float32)
        key_sum = key_sum + lax.dot_general(coef, operands[0], (((0,), (0,)), ((), ())), preferred_element_type=jnp.float32)
        return (key_sum, anchor_part)
    key_sum, anchor_parts = lax.scan(grad_step, jnp.zeros((view_count, width), jnp.float32), blocked + blocked_stats)
    grad = anchor_parts.reshape(view_count, width) + key_sum
    along = lax.optimization_barrier(jnp.sum(unit_student * grad, axis=1, keepdims=True))
    feature_grad = scaling * (grad - unit_student * along)
    return (jnp.mean(contrast), jnp.mean(relation), feature_grad)
```

```python
import math

import jax
import jax.numpy as jnp
from jax import lax
from jax.experimental import pallas as pl
from jax.experimental.pallas import tpu as pltpu
from jax.sharding import Mesh
from jax.sharding import PartitionSpec as P

AXES = ("x_lo", "core", "z", "x_hi", "y")
MESH = pl.DeviceIdType.MESH
F32, BF16 = jnp.float32, jnp.bfloat16

temp_sup = 0.1
temp_student = 0.2
temp_teacher = 0.05
epsilon = 1e-06
LOG2E = math.log2(math.e)

KEY_POS = {2: 0, 1: 1, 3: 2, 0: 3}
RING = (1, 2, 3)


def plane_messages():
    out = {}
    out["u", (1, 0)] = ((0, 0), "y", -1)
    out["u", (3, 0)] = ((0, 0), "y", 1)
    out["v", (0, 1)] = ((0, 0), "z", -1)
    out["v", (0, 3)] = ((0, 0), "z", 1)
    out["u", (2, 0)] = ((1, 0), "y", -1)
    out["v", (0, 2)] = ((0, 3), "z", 1)
    for d in range(4):
        out["u", (d, 1)] = ((d, 0), "z", -1)
        out["u", (d, 3)] = ((d, 0), "z", 1)
        out["u", (d, 2)] = ((d, 1), "z", -1) if d in (0, 3) else ((d, 3), "z", 1)
        out["v", (1, d)] = ((0, d), "y", -1)
        out["v", (3, d)] = ((0, d), "y", 1)
        out["v", (2, d)] = ((1, d), "y", -1) if d in (3,) else ((3, d), "y", 1)
    return out


def line_messages():
    return {
        ("ku", 1): (0, "x", -1),
        ("ku", 3): (0, "x", 1),
        ("kv", 1): (0, "x", -1),
        ("kv", 3): (0, "x", 1),
        ("ku", 2): (1, "x", -1),
        ("kv", 2): (3, "x", 1),
    }


def make_schedule():
    wire, hop, tile, local = 5.6, 2.2, 1.3, 1.4
    messages = {**plane_messages(), **line_messages()}
    free = {}
    arrive = {}

    def launch(name, when):
        _, axis, step = messages[name]
        begin = max(free.get((axis, step), 0.0), when)
        free[axis, step] = begin + wire
        arrive[name] = begin + wire + hop

    def after(kind, slot):
        return [n for n, m in messages.items() if n[0] == kind and m[0] == slot]

    first = []
    for kind, own in (("u", (0, 0)), ("v", (0, 0)), ("ku", 0), ("kv", 0)):
        first += after(kind, own)
    order = {n: i for i, n in enumerate(messages)}
    first.sort(key=lambda n: order[n])
    for name in first:
        launch(name, 0.0)
    now, waited, done_tiles = 0.0, {}, []
    sequence = [("launch", tuple(first))]
    pending_actions = []
    steps = []
    slots = [(dy, dz) for dz in range(4) for dy in range(4)]
    have = {("u", (0, 0)): 0.0, ("v", (0, 0)): 0.0}
    while len(done_tiles) < 16:
        coming = sorted((t, order[n], n) for n, t in arrive.items() if n not in waited)
        keys_in = all(n in waited for n in line_messages())
        ready = []
        if keys_in:
            ready = [
                s
                for s in slots
                if s not in done_tiles
                and all((k, s) in have and have[k, s] + local <= now for k in ("u", "v"))
            ]
        if coming and coming[0][0] <= now or (coming and not ready):
            t, _, name = coming[0]
            now = max(now, t) + 0.05
            waited[name] = now
            follow = after(name[0], name[1])
            for f in follow:
                launch(f, now)
            if name[0] in ("u", "v"):
                have[name] = now
            pending_actions.append((name, tuple(follow)))
        elif ready:
            ready.sort(key=lambda s: (max(have["u", s], have["v", s]), slots.index(s)))
            done_tiles.append(ready[0])
            steps.append(tuple(pending_actions))
            pending_actions = []
            now += tile
        else:
            now = min(
                max(have["u", s], have["v", s]) + local + 1e-6
                for s in slots
                if s not in done_tiles and ("u", s) in have and ("v", s) in have
            )
    return tuple(first), tuple(steps), tuple(done_tiles), now


FIRST, STEPS, TILES, _ = make_schedule()
SLOT = {s: k for k, s in enumerate(TILES)}
MESSAGES = {**plane_messages(), **line_messages()}
NAMES = (
    list(MESSAGES)
    + [("pu", s) for s in TILES]
    + [("pv", s) for s in TILES]
    + [(kind, d) for kind in ("lx", "ly", "lz", "sx", "sy", "sz", "ox") for d in RING]
    + [("lp", 0), ("sp", 0)]
    + [("r", i) for i in range(6)]
)
IDS = {n: i for i, n in enumerate(NAMES)}


def kernel(
    student_ref,
    teacher_ref,
    label_ref,
    grad_ref,
    loss_ref,
    ua,
    va,
    uk,
    vk,
    raw_s,
    raw_t,
    signed_b,
    w_all,
    acc,
    key_label,
    anchor_label,
    label_plane,
    label_line,
    part,
    part_in,
    coef_plane,
    key_coef,
    anchor_coef,
    loss_line,
    gbuf,
    total,
    relay,
    arrive,
    send_sem,
    recv_sem,
):
    rows, width = student_ref.shape
    x_lo, x_hi = lax.axis_index("x_lo"), lax.axis_index("x_hi")
    core = lax.axis_index("core")
    y, z = lax.axis_index("y"), lax.axis_index("z")
    x = x_hi * 2 + x_lo
    pair = 2 * rows

    def device(axis, step):
        if axis == "core":
            return {"core": 1 - core}
        if axis == "x":
            there = lax.rem(x + step + 4, 4)
            return {"x_hi": there // 2, "x_lo": lax.rem(there, 2)}
        place = y if axis == "y" else z
        return {axis: lax.rem(place + step + 4, 4)}

    def key_rows(d):
        return pl.ds(KEY_POS[d] * rows, rows)

    def own_rows(slot):
        return pl.ds(SLOT[slot] * pair, rows)

    half = rows // 2

    def refs_of(name):
        kind, slot = name
        if kind in ("u", "v"):
            source, axis, step = MESSAGES[name]
            buf = ua if kind == "u" else va
            return buf.at[own_rows(source)], buf.at[own_rows(slot)], axis, step
        if kind in ("ku", "kv"):
            source, axis, step = MESSAGES[name]
            buf = uk if kind == "ku" else vk
            return buf.at[key_rows(source)], buf.at[key_rows(slot)], axis, step
        if kind in ("pu", "pv"):
            buf = ua if kind == "pu" else va
            there = pl.ds(SLOT[slot] * pair + rows, rows)
            return buf.at[own_rows(slot)], buf.at[there], "core", 0
        if kind in ("lx", "ox"):
            buf = label_line if kind == "lx" else loss_line
            return buf.at[0], buf.at[slot], "x", -slot
        if kind == "sx":
            return part, part_in.at[slot - 1], "x", -slot
        plane = label_plane if kind[0] == "l" else coef_plane
        if kind in ("ly", "sy"):
            return plane.at[0, 0, 0], plane.at[0, 0, slot], "y", -slot
        if kind in ("lz", "sz"):
            return plane.at[0, 0], plane.at[0, slot], "z", -slot
        if kind in ("lp", "sp"):
            return plane.at[0], plane.at[1], "core", 0
        two, nxt, prv = KEY_POS[2] * rows, KEY_POS[1] * rows, KEY_POS[3] * rows
        return (
            (total.at[pl.ds(two, half)], relay.at[0], "x", 1),
            (total.at[pl.ds(two + half, half)], relay.at[1], "x", -1),
            (total.at[pl.ds(nxt + half, half)], arrive.at[0, pl.ds(half, half)], "x", 1),
            (total.at[pl.ds(prv, half)], arrive.at[1, pl.ds(0, half)], "x", -1),
            (total.at[pl.ds(nxt, half)], arrive.at[0, pl.ds(0, half)], "x", 1),
            (total.at[pl.ds(prv + half, half)], arrive.at[1, pl.ds(half, half)], "x", -1),
        )[slot]

    def message(name):
        source, target, axis, step = refs_of(name)
        return pltpu.make_async_remote_copy(
            src_ref=source,
            dst_ref=target,
            send_sem=send_sem.at[IDS[name]],
            recv_sem=recv_sem.at[IDS[name]],
            device_id=device(axis, step),
            device_id_type=MESH,
        )

    def start(*names):
        for name in names:
            message(name).start()

    def arrived(*names):
        for name in names:
            message(name).wait_recv()

    barrier = pltpu.get_barrier_semaphore()
    for axis in ("x", "y", "z"):
        for d in RING:
            pl.semaphore_signal(barrier, inc=1, device_id=device(axis, d), device_id_type=MESH)
    pl.semaphore_signal(barrier, inc=1, device_id=device("core", 0), device_id_type=MESH)

    own_key = KEY_POS[0] * rows

    def normalise(i, carry):
        here = pl.ds(pl.multiple_of(i * 16, 16), 16)
        there = pl.ds(pl.multiple_of(own_key + i * 16, 16), 16)
        for raw, anchors, keys in ((student_ref, ua, uk), (teacher_ref, va, vk)):
            values = raw[here, :].astype(F32)
            scaling = lax.rsqrt(jnp.sum(values * values, axis=1, keepdims=True) + epsilon)
            unit = (values * scaling).astype(BF16)
            anchors[here, :] = unit
            keys[there, :] = unit
        return carry

    lax.fori_loop(0, rows // 16, normalise, 0)
    own_label = jnp.broadcast_to(label_ref[...].astype(F32), (8, rows))
    label_plane[0, 0, 0] = own_label
    label_line[0] = own_label
    acc[...] = jnp.zeros_like(acc)
    pl.semaphore_wait(barrier, 10)

    start(*[("ly", d) for d in RING], *[("lx", d) for d in RING])
    start(*FIRST)
    start(("pu", (0, 0)), ("pv", (0, 0)))
    arrived(*[("ly", d) for d in RING])
    start(*[("lz", d) for d in RING])
    arrived(*[("lx", d) for d in RING])
    for d in range(4):
        line = label_line[d][0:1]
        key_label[key_rows(d), :] = jnp.broadcast_to(line, (rows, rows)).T
    arrived(*[("lz", d) for d in RING])
    start(("lp", 0))
    arrived(("lp", 0))
    for (dy, dz), k in SLOT.items():
        for c in range(2):
            anchor_label[:, pl.ds(k * pair + c * rows, rows)] = label_plane[c, dz, dy]

    chunk = 32
    k_rel = LOG2E / temp_student
    k_tea = LOG2E / temp_teacher

    def elementwise(k, count, base, diagonal):
        def one(i, carry):
            r = pl.ds(pl.multiple_of(base + i * chunk, chunk), chunk)
            label = key_label[r, :]
            sums = [None] * 6
            for c in range(2):
                lanes = pl.ds(c * rows, rows)
                columns = pl.ds(pl.multiple_of(k * pair + c * rows, rows), rows)
                s = raw_s[r, lanes]
                t = raw_t[r, lanes]
                b = jnp.exp2(s * k_rel - k_rel)
                w = jnp.exp2(t * k_tea - k_tea)
                same = label == jnp.broadcast_to(anchor_label[0:1, columns], label.shape)
                if diagonal and c == 0:
                    row = lax.broadcasted_iota(jnp.int32, label.shape, 0) + i * chunk
                    lane = lax.broadcasted_iota(jnp.int32, label.shape, 1)
                    other = row != lane
                    same = jnp.logical_and(same, other)
                    b = jnp.where(other, b, 0.0)
                    w = jnp.where(other, w, 0.0)
                signed_b[r, columns] = jnp.where(same, -b, b)
                w_all[r, columns] = w
                values = (b * b, b, w, w * s, jnp.where(same, s, 0.0), jnp.where(same, 1.0, 0.0))
                sums = [v if p is None else p + v for p, v in zip(sums, values)]
            for n in range(6):
                acc[n, r, :] += sums[n]
            return carry

        lax.fori_loop(0, count // chunk, one, 0)

    key_count = 4 * rows
    contract = (((1,), (1,)), ((), ()))

    def tile_step(k, carry):
        for n, actions in enumerate(STEPS):
            @pl.when(k == n)
            def _(n=n, actions=actions):
                for name, follow in actions:
                    arrived(name)
                    start(*follow)
                    if name[0] in ("u", "v"):
                        start(("p" + name[0], name[1]))
                arrived(("pu", TILES[n]), ("pv", TILES[n]))

        here = pl.ds(pl.multiple_of(k * pair, pair), pair)
        raw_s[...] = lax.dot_general(uk[...], ua[here, :], contract, preferred_element_type=F32)
        raw_t[...] = lax.dot_general(vk[...], va[here, :], contract, preferred_element_type=F32)
        elementwise(k, key_count - rows, 0, False)

        @pl.when(k == 0)
        def _():
            elementwise(k, rows, own_key, True)

        @pl.when(k > 0)
        def _():
            elementwise(k, rows, own_key, False)

        return carry

    lax.fori_loop(0, 16, tile_step, 0)

    lane = lax.broadcasted_iota(jnp.int32, (rows, rows), 1)
    for d in range(4):
        packed = jnp.zeros((rows, rows), F32)
        for n in range(6):
            packed = jnp.where(
                lane == n, jnp.sum(acc[n, key_rows(d), :], axis=1, keepdims=True), packed
            )
        part[d] = packed.T[0:8]
    start(*[("sx", d) for d in RING])
    arrived(*[("sx", d) for d in RING])
    line = lax.broadcasted_iota(jnp.int32, (8, rows), 0)
    for e in range(4):
        sums = part[e]
        for d in RING:
            sums = sums + part_in[d - 1, (e - d) % 4]
        sup, rel, tea = sums[0:1], sums[1:2], sums[2:3]
        positives = jnp.maximum(sums[5:6], 1.0)
        coefs = (
            (1.0 / temp_sup) / sup,
            (1.0 / temp_student) / rel,
            (1.0 / temp_student) / tea,
            (1.0 / temp_sup) / positives,
        )
        for n in range(4):
            key_coef[n, key_rows(e), :] = jnp.broadcast_to(coefs[n], (rows, rows)).T
        if e == 0:
            contrast = (1.0 - sums[4:5] / positives) / temp_sup + jnp.log(sup)
            relation = (1.0 - sums[3:4] / tea) / temp_student + jnp.log(rel)
            mine = jnp.zeros((8, rows), F32)
            for n, value in enumerate((*coefs, contrast, relation)):
                mine = jnp.where(line == n, jnp.broadcast_to(value, (8, rows)), mine)
            coef_plane[0, 0, 0] = mine
            start(*[("sy", d) for d in RING])

    depth = 4 * rows
    chunks = 32 * rows // depth

    def fill(c, first, count, side):
        def one(i, carry):
            r = pl.ds(pl.multiple_of(first + i * chunk, chunk), chunk)
            g = pl.ds(pl.multiple_of(i * chunk, chunk), chunk)
            for q in range(depth // rows):
                columns = pl.ds(pl.multiple_of(c * depth + q * rows, rows), rows)
                sb = signed_b[r, columns]
                w = w_all[r, columns]
                if side == "key":
                    ca, cb, cw, cp = [key_coef[n, r, :] for n in range(4)]
                else:
                    ca, cb, cw, cp = [
                        jnp.broadcast_to(anchor_coef[n : n + 1, columns], sb.shape)
                        for n in range(4)
                    ]
                value = (sb * sb * ca - jnp.where(sb < 0.0, cp, 0.0)) + (
                    jnp.abs(sb) * cb - w * cw
                )
                gbuf[g, pl.ds(q * rows, rows)] = value.astype(BF16)
            return carry

        lax.fori_loop(0, count // chunk, one, 0)

    def multiply(c, first, count, fresh):
        anchors = ua[pl.ds(pl.multiple_of(c * depth, depth), depth), :]
        product = jnp.dot(gbuf[pl.ds(0, count), :], anchors, preferred_element_type=F32)
        if fresh:
            total[pl.ds(first, count), :] = product
        else:
            total[pl.ds(first, count), :] += product

    def key_side(c, carry):
        @pl.when(c == 2)
        def _():
            arrived(*[("sy", d) for d in RING])
            start(*[("sz", d) for d in RING])

        @pl.when(c == 5)
        def _():
            arrived(*[("sz", d) for d in RING])
            start(("sp", 0))

        fill(c, 0, key_count, "key")
        multiply(c, 0, key_count, False)
        return carry

    total[...] = jnp.zeros_like(total)
    lax.fori_loop(0, chunks, key_side, 0)
    arrived(("sp", 0))
    for (dy, dz), k in SLOT.items():
        for c in range(2):
            anchor_coef[:, pl.ds(k * pair + c * rows, rows)] = coef_plane[c, dz, dy]
    losses = jnp.zeros((8, rows), F32)
    for cc in range(2):
        for zz in range(4):
            for yy in range(4):
                losses = losses + coef_plane[
                    lax.rem(cc + core, 2), lax.rem(zz + 4 - z, 4), lax.rem(yy + 4 - y, 4)
                ]
    loss_line[0] = losses
    start(*[("ox", d) for d in RING])

    def anchor_side(first, count):
        def one(c, carry):
            fill(c, first, count, "anchor")
            multiply(c, first, count, False)
            return carry

        lax.fori_loop(0, chunks, one, 0)

    anchor_side(0, rows)
    start(("r", 0), ("r", 1))
    anchor_side(rows, 2 * rows)
    start(("r", 2), ("r", 3))
    arrived(("r", 0))
    total[pl.ds(KEY_POS[1] * rows, half), :] += relay[0]
    start(("r", 4))
    arrived(("r", 1))
    total[pl.ds(KEY_POS[3] * rows + half, half), :] += relay[1]
    start(("r", 5))
    anchor_side(own_key, rows)

    arrived(*[("ox", d) for d in RING])
    sums = jnp.zeros((8, rows), F32)
    for xx in range(4):
        sums = sums + loss_line[lax.rem(xx + 4 - x, 4)]
    views = 128.0 * rows
    loss_ref[...] = jnp.broadcast_to(jnp.sum(sums, axis=1, keepdims=True), (8, rows)) / views

    arrived(("r", 2), ("r", 3), ("r", 4), ("r", 5))

    def finish(i, carry):
        here = pl.ds(pl.multiple_of(i * 16, 16), 16)
        there = pl.ds(pl.multiple_of(own_key + i * 16, 16), 16)
        values = student_ref[here, :].astype(F32)
        scaling = lax.rsqrt(jnp.sum(values * values, axis=1, keepdims=True) + epsilon)
        unit = values * scaling
        grad = total[there, :] + arrive[0, here, :] + arrive[1, here, :]
        along = jnp.sum(unit * grad, axis=1, keepdims=True)
        grad_ref[here, :] = scaling * (grad - unit * along)
        return carry

    lax.fori_loop(0, rows // 16, finish, 0)
    for name in NAMES:
        message(name).wait_send()


def body(student, teacher, labels):
    rows, width = student.shape
    keys, anchors = 4 * rows, 32 * rows
    vmem = pl.BlockSpec(memory_space=pltpu.VMEM)
    grad, losses = pl.pallas_call(
        kernel,
        out_shape=(
            jax.ShapeDtypeStruct((rows, width), F32),
            jax.ShapeDtypeStruct((8, rows), F32),
        ),
        in_specs=[vmem] * 3,
        out_specs=(vmem, vmem),
        scratch_shapes=[
            pltpu.VMEM((anchors, width), BF16),
            pltpu.VMEM((anchors, width), BF16),
            pltpu.VMEM((keys, width), BF16),
            pltpu.VMEM((keys, width), BF16),
            pltpu.VMEM((keys, 2 * rows), F32),
            pltpu.VMEM((keys, 2 * rows), F32),
            pltpu.VMEM((keys, anchors), F32),
            pltpu.VMEM((keys, anchors), F32),
            pltpu.VMEM((6, keys, rows), F32),
            pltpu.VMEM((keys, rows), F32),
            pltpu.VMEM((8, anchors), F32),
            pltpu.VMEM((2, 4, 4, 8, rows), F32),
            pltpu.VMEM((4, 8, rows), F32),
            pltpu.VMEM((4, 8, rows), F32),
            pltpu.VMEM((3, 4, 8, rows), F32),
            pltpu.VMEM((2, 4, 4, 8, rows), F32),
            pltpu.VMEM((4, keys, rows), F32),
            pltpu.VMEM((8, anchors), F32),
            pltpu.VMEM((4, 8, rows), F32),
            pltpu.VMEM((keys, 4 * rows), BF16),
            pltpu.VMEM((keys, width), F32),
            pltpu.VMEM((2, rows // 2, width), F32),
            pltpu.VMEM((2, rows, width), F32),
            pltpu.SemaphoreType.DMA((len(NAMES),)),
            pltpu.SemaphoreType.DMA((len(NAMES),)),
        ],
        compiler_params=pltpu.CompilerParams(
            collective_id=0, has_side_effects=True, vmem_limit_bytes=60 * 1024 * 1024
        ),
    )(student, teacher, labels.reshape(1, rows))
    return losses[4, 0], losses[5, 0], grad


def solution(mesh):
    torus = Mesh(mesh.devices.reshape(2, 2, 4, 2, 4), AXES)
    own = ("x_lo", "core", "z", "x_hi", "y")
    return jax.shard_map(
        body,
        mesh=torus,
        in_specs=(P(own, None), P(own, None), P(own)),
        out_specs=(P(), P(), P(own, None)),
        check_vma=False,
    )
```

```python
import math

import jax
import jax.numpy as jnp
from jax import lax
from jax.experimental import pallas as pl
from jax.experimental.pallas import tpu as pltpu
from jax.sharding import Mesh
from jax.sharding import PartitionSpec as P

AXES = ("x_lo", "core", "z", "x_hi", "y")
MESH = pl.DeviceIdType.MESH
F32, BF16 = jnp.float32, jnp.bfloat16

temp_sup = 0.1
temp_student = 0.2
temp_teacher = 0.05
epsilon = 1e-06
LOG2E = math.log2(math.e)

KEY_POS = {2: 0, 1: 1, 3: 2, 0: 3}
RING = (1, 2, 3)
OTHERS = [(dy, dz) for dz in range(4) for dy in range(4) if (dy, dz) != (0, 0)]


def plane_messages():
    out = {}
    near = ((1, -1), (3, 1))

    def along(kind, axis, others):
        for d, step in near:
            for o in others:
                slot, source = ((d, o), (0, o)) if axis == "y" else ((o, d), (o, 0))
                for h in range(2):
                    out[kind, slot, h] = (source, axis, step)
        for o in others:
            for h, (d, step) in enumerate(near):
                slot, source = ((2, o), (d, o)) if axis == "y" else ((o, 2), (o, d))
                out[kind, slot, h] = (source, axis, step)

    along("u", "y", (0,))
    along("v", "z", (0,))
    along("u", "z", range(4))
    along("v", "y", range(4))
    return out


def line_messages():
    out = {}
    for kind in ("ku", "kv"):
        for d, step in ((1, -1), (3, 1)):
            for h in range(2):
                out[kind, d, h] = (0, "x", step)
        for h, (d, step) in enumerate(((1, -1), (3, 1))):
            out[kind, 2, h] = (d, "x", step)
    return out


MESSAGES = {**plane_messages(), **line_messages()}


PRIORITY = (
    62, 23, 50, 16, 52, 27, 0, 32, 58, 39, 6, 33, 66, 43, 60, 68, 13, 7,
    10, 56, 5, 49, 38, 18, 51, 54, 15, 1, 35, 46, 2, 55, 19, 29, 71, 44,
    64, 53, 59, 8, 37, 28, 67, 63, 70, 45, 47, 69, 17, 65, 3, 14, 30, 9,
    31, 36, 61, 4, 41, 11, 12, 48, 42, 22, 34, 40, 21, 24, 20, 25, 26, 57,
)


def make_schedule():
    wire, hop, tile, local = 2.8, 2.2, 1.4, 1.5
    order = dict(zip(MESSAGES, PRIORITY))
    free, arrive, waited, have = {}, {}, {}, {}

    def launch(name, when):
        _, axis, step = MESSAGES[name]
        free[axis, step] = max(free.get((axis, step), 0.0), when) + wire
        arrive[name] = free[axis, step] + hop

    def after(kind, slot, half):
        found = [
            n for n, m in MESSAGES.items() if n[0] == kind and m[0] == slot and n[2] == half
        ]
        return tuple(sorted(found, key=order.get))

    own = (("u", (0, 0)), ("v", (0, 0)), ("ku", 0), ("kv", 0))
    first = sorted((n for k in own for h in range(2) for n in after(*k, h)), key=order.get)
    for name in first:
        launch(name, 0.0)
    slots = [(dy, dz) for dz in range(4) for dy in range(4)]
    whole = {("u", (0, 0)): 0.0, ("v", (0, 0)): 0.0}
    now, tiles, steps, actions = 0.0, [], [], []
    lines = list(line_messages())

    def ready_at(slot):
        return max(whole.get((k, slot), 1e9) for k in ("u", "v")) + local

    while len(tiles) < 16:
        coming = min(((t, order[n], n) for n, t in arrive.items() if n not in waited), default=None)
        able = [s for s in slots if s not in tiles and ready_at(s) <= now]
        if not all(n in waited for n in lines):
            able = []
        if coming and (coming[0] <= now or not able):
            now = max(now, coming[0]) + 0.05
            name = coming[2]
            waited[name] = now
            follow = after(*name)
            for f in follow:
                launch(f, now)
            kind, slot, half = name
            complete = (kind, slot, 1 - half) in waited
            if complete:
                whole[kind, slot] = now
            actions.append((name, follow, complete and kind in ("u", "v")))
        elif able:
            best = min(able, key=lambda s: (ready_at(s), slots.index(s)))
            tiles.append(best)
            steps.append(tuple(actions))
            actions = []
            now += tile
        else:
            now = min(ready_at(s) for s in slots if s not in tiles) + 1e-6
    return tuple(first), tuple(steps), tuple(tiles), now


FIRST, STEPS, TILES, _ = make_schedule()
SLOT = {s: k for k, s in enumerate(TILES)}
NAMES = (
    list(MESSAGES)
    + [("pu", s) for s in TILES]
    + [("pv", s) for s in TILES]
    + [(kind, d) for kind in ("lx", "sx", "ox") for d in RING]
    + [(kind, o) for kind in ("l", "s") for o in OTHERS]
    + [("lp", 0), ("sp", 0)]
    + [("r", i) for i in range(6)]
)
IDS = {n: i for i, n in enumerate(NAMES)}


def kernel(
    student_ref,
    teacher_ref,
    label_ref,
    grad_ref,
    loss_ref,
    ua,
    va,
    uk,
    vk,
    raw_s,
    raw_t,
    signed_b,
    w_all,
    acc,
    key_label,
    anchor_label,
    label_plane,
    label_line,
    part,
    part_in,
    coef_plane,
    key_coef,
    anchor_coef,
    loss_line,
    gbuf0,
    gbuf1,
    total,
    relay,
    arrive,
    send_sem,
    recv_sem,
):
    rows, width = student_ref.shape
    x_lo, x_hi = lax.axis_index("x_lo"), lax.axis_index("x_hi")
    core = lax.axis_index("core")
    y, z = lax.axis_index("y"), lax.axis_index("z")
    x = x_hi * 2 + x_lo
    pair = 2 * rows

    def device(axis, step):
        if axis == "core":
            return {"core": 1 - core}
        if axis == "x":
            there = lax.rem(x + step + 4, 4)
            return {"x_hi": there // 2, "x_lo": lax.rem(there, 2)}
        if axis == "plane":
            dy, dz = step
            return {"y": lax.rem(y + 4 - dy, 4), "z": lax.rem(z + 4 - dz, 4)}
        place = y if axis == "y" else z
        return {axis: lax.rem(place + step + 4, 4)}

    def key_rows(d):
        return pl.ds(KEY_POS[d] * rows, rows)

    def own_rows(slot):
        return pl.ds(SLOT[slot] * pair, rows)

    half = rows // 2

    def part_of(start, h):
        return pl.ds(start + h * half, half)

    def refs_of(name):
        kind, slot = name[:2]
        if kind in ("u", "v"):
            source, axis, step = MESSAGES[name]
            buf = ua if kind == "u" else va
            here, there = SLOT[source] * pair, SLOT[slot] * pair
            return buf.at[part_of(here, name[2])], buf.at[part_of(there, name[2])], axis, step
        if kind in ("ku", "kv"):
            source, axis, step = MESSAGES[name]
            buf = uk if kind == "ku" else vk
            here, there = KEY_POS[source] * rows, KEY_POS[slot] * rows
            return buf.at[part_of(here, name[2])], buf.at[part_of(there, name[2])], axis, step
        if kind in ("pu", "pv"):
            buf = ua if kind == "pu" else va
            there = pl.ds(SLOT[slot] * pair + rows, rows)
            return buf.at[own_rows(slot)], buf.at[there], "core", 0
        if kind in ("lx", "ox"):
            buf = label_line if kind == "lx" else loss_line
            return buf.at[0], buf.at[slot], "x", -slot
        if kind == "sx":
            return part, part_in.at[slot - 1], "x", -slot
        plane = label_plane if kind[0] == "l" else coef_plane
        if kind in ("l", "s"):
            return plane.at[0, 0, 0], plane.at[0, slot[1], slot[0]], "plane", slot
        if kind in ("lp", "sp"):
            return plane.at[0], plane.at[1], "core", 0
        two, nxt, prv = KEY_POS[2] * rows, KEY_POS[1] * rows, KEY_POS[3] * rows
        return (
            (total.at[pl.ds(two, half)], relay.at[0], "x", 1),
            (total.at[pl.ds(two + half, half)], relay.at[1], "x", -1),
            (total.at[pl.ds(nxt + half, half)], arrive.at[0, pl.ds(half, half)], "x", 1),
            (total.at[pl.ds(prv, half)], arrive.at[1, pl.ds(0, half)], "x", -1),
            (total.at[pl.ds(nxt, half)], arrive.at[0, pl.ds(0, half)], "x", 1),
            (total.at[pl.ds(prv + half, half)], arrive.at[1, pl.ds(half, half)], "x", -1),
        )[slot]

    def message(name):
        source, target, axis, step = refs_of(name)
        return pltpu.make_async_remote_copy(
            src_ref=source,
            dst_ref=target,
            send_sem=send_sem.at[IDS[name]],
            recv_sem=recv_sem.at[IDS[name]],
            device_id=device(axis, step),
            device_id_type=MESH,
        )

    def start(*names):
        for name in names:
            message(name).start()

    def arrived(*names):
        for name in names:
            message(name).wait_recv()

    barrier = pltpu.get_barrier_semaphore()
    for axis, steps in (("x", RING), ("plane", OTHERS)):
        for d in steps:
            pl.semaphore_signal(barrier, inc=1, device_id=device(axis, d), device_id_type=MESH)
    pl.semaphore_signal(barrier, inc=1, device_id=device("core", 0), device_id_type=MESH)

    own_key = KEY_POS[0] * rows

    def normalise(i, carry):
        here = pl.ds(pl.multiple_of(i * 16, 16), 16)
        there = pl.ds(pl.multiple_of(own_key + i * 16, 16), 16)
        for raw, anchors, keys in ((student_ref, ua, uk), (teacher_ref, va, vk)):
            values = raw[here, :].astype(F32)
            scaling = lax.rsqrt(jnp.sum(values * values, axis=1, keepdims=True) + epsilon)
            unit = (values * scaling).astype(BF16)
            anchors[here, :] = unit
            keys[there, :] = unit
        return carry

    lax.fori_loop(0, rows // 16, normalise, 0)
    own_label = jnp.broadcast_to(label_ref[...].astype(F32), (8, rows))
    label_plane[0, 0, 0] = own_label
    label_line[0] = own_label
    acc[...] = jnp.zeros_like(acc)
    total[...] = jnp.zeros_like(total)
    pl.semaphore_wait(barrier, 19)

    start(*[("l", o) for o in OTHERS], *[("lx", d) for d in RING])
    start(*FIRST)
    start(("pu", (0, 0)), ("pv", (0, 0)))

    def labels_in():
        arrived(("lp", 0), *[("lx", d) for d in RING])
        for d in range(4):
            line = label_line[d][0:1]
            key_label[key_rows(d), :] = jnp.broadcast_to(line, (rows, rows)).T
        for (dy, dz), k in SLOT.items():
            for c in range(2):
                anchor_label[:, pl.ds(k * pair + c * rows, rows)] = label_plane[c, dz, dy]

    chunk = 32
    k_rel = LOG2E / temp_student
    k_tea = LOG2E / temp_teacher

    def elementwise(k, count, base, diagonal):
        def one(i, carry):
            r = pl.ds(pl.multiple_of(base + i * chunk, chunk), chunk)
            label = key_label[r, :]
            sums = [None] * 6
            for c in range(2):
                lanes = pl.ds(c * rows, rows)
                columns = pl.ds(pl.multiple_of(k * pair + c * rows, rows), rows)
                s = raw_s[r, lanes]
                t = raw_t[r, lanes]
                b = jnp.exp2(s * k_rel - k_rel)
                w = jnp.exp2(t * k_tea - k_tea)
                same = label == jnp.broadcast_to(anchor_label[0:1, columns], label.shape)
                if diagonal and c == 0:
                    row = lax.broadcasted_iota(jnp.int32, label.shape, 0) + i * chunk
                    lane = lax.broadcasted_iota(jnp.int32, label.shape, 1)
                    other = row != lane
                    same = jnp.logical_and(same, other)
                    b = jnp.where(other, b, 0.0)
                    w = jnp.where(other, w, 0.0)
                signed_b[r, columns] = jnp.where(same, -b, b)
                w_all[r, columns] = w
                values = (b * b, b, w, w * s, jnp.where(same, s, 0.0), jnp.where(same, 1.0, 0.0))
                sums = [v if p is None else p + v for p, v in zip(sums, values)]
            for n in range(6):
                acc[n, r, :] += sums[n]
            return carry

        lax.fori_loop(0, count // chunk, one, 0)

    key_count = 4 * rows
    contract = (((1,), (1,)), ((), ()))

    def tile_step(k, carry):
        for n, actions in enumerate(STEPS):
            @pl.when(k == n)
            def _(n=n, actions=actions):
                for i, (name, follow, complete) in enumerate(actions):
                    if n == 0 and i == 10:
                        arrived(*[("l", o) for o in OTHERS])
                        start(("lp", 0))
                    arrived(name)
                    start(*follow)
                    if complete:
                        start(("p" + name[0], name[1]))
                arrived(("pu", TILES[n]), ("pv", TILES[n]))
                if n == 0:
                    labels_in()

        here = pl.ds(pl.multiple_of(k * pair, pair), pair)
        raw_s[...] = lax.dot_general(uk[...], ua[here, :], contract, preferred_element_type=F32)
        raw_t[...] = lax.dot_general(vk[...], va[here, :], contract, preferred_element_type=F32)
        elementwise(k, key_count - rows, 0, False)

        @pl.when(k == 0)
        def _():
            elementwise(k, rows, own_key, True)

        @pl.when(k > 0)
        def _():
            elementwise(k, rows, own_key, False)

        return carry

    lax.fori_loop(0, 16, tile_step, 0)

    lane = lax.broadcasted_iota(jnp.int32, (rows, rows), 1)
    for d in range(4):
        packed = jnp.zeros((rows, rows), F32)
        for n in range(6):
            packed = jnp.where(
                lane == n, jnp.sum(acc[n, key_rows(d), :], axis=1, keepdims=True), packed
            )
        part[d] = packed.T[0:8]
    start(*[("sx", d) for d in RING])
    arrived(*[("sx", d) for d in RING])
    line = lax.broadcasted_iota(jnp.int32, (8, rows), 0)

    def coefficients(e):
        sums = part[e]
        for d in RING:
            sums = sums + part_in[d - 1, (e - d) % 4]
        sup, rel, tea = sums[0:1], sums[1:2], sums[2:3]
        positives = jnp.maximum(sums[5:6], 1.0)
        coefs = (
            (1.0 / temp_sup) / sup,
            (1.0 / temp_student) / rel,
            (1.0 / temp_student) / tea,
            (1.0 / temp_sup) / positives,
        )
        if e == 0:
            contrast = (1.0 - sums[4:5] / positives) / temp_sup + jnp.log(sup)
            relation = (1.0 - sums[3:4] / tea) / temp_student + jnp.log(rel)
            mine = jnp.zeros((8, rows), F32)
            for n, value in enumerate((*coefs, contrast, relation)):
                mine = jnp.where(line == n, jnp.broadcast_to(value, (8, rows)), mine)
            coef_plane[0, 0, 0] = mine
            start(*[("s", o) for o in OTHERS])
        for n in range(4):
            key_coef[n, key_rows(e), :] = jnp.broadcast_to(coefs[n], (rows, rows)).T

    depth = 4 * rows
    chunks = 32 * rows // depth

    def fill(c, first, count, sides, out):
        for i in range(count // chunk):
            r = pl.ds(first + i * chunk, chunk)
            for q in range(depth // rows):
                columns = pl.ds(pl.multiple_of(c * depth + q * rows, rows), rows)
                sb = signed_b[r, columns]
                w = w_all[r, columns]
                b, a, positive = jnp.abs(sb), sb * sb, sb < 0.0
                for n, side in enumerate(sides):
                    if side == "key":
                        ca, cb, cw, cp = [key_coef[m, r, :] for m in range(4)]
                    else:
                        ca, cb, cw, cp = [
                            jnp.broadcast_to(anchor_coef[m : m + 1, columns], sb.shape)
                            for m in range(4)
                        ]
                    value = (a * ca - jnp.where(positive, cp, 0.0)) + (b * cb - w * cw)
                    out[pl.ds(n * count + i * chunk, chunk), pl.ds(q * rows, rows)] = value.astype(
                        BF16
                    )

    def multiply(c, first, count, sides, out):
        anchors = ua[pl.ds(pl.multiple_of(c * depth, depth), depth), :]
        made = out[pl.ds(0, count * len(sides)), :]
        product = jnp.dot(made, anchors, preferred_element_type=F32)
        if len(sides) == 2:
            product = product[0:count] + product[count : 2 * count]
        total[pl.ds(first, count), :] += product

    def second_pass(first, count, sides):
        fill(0, first, count, sides, gbuf0)

        def one(j, carry):
            c = 2 * j
            multiply(c, first, count, sides, gbuf0)
            fill(c + 1, first, count, sides, gbuf1)
            multiply(c + 1, first, count, sides, gbuf1)
            fill(jnp.minimum(c + 2, chunks - 1), first, count, sides, gbuf0)
            return carry

        lax.fori_loop(0, chunks // 2, one, 0)

    coefficients(0)
    coefficients(2)
    second_pass(0, rows, ("key",))
    arrived(*[("s", o) for o in OTHERS])
    start(("sp", 0))
    coefficients(1)
    coefficients(3)
    arrived(("sp", 0))
    for (dy, dz), k in SLOT.items():
        for c in range(2):
            anchor_coef[:, pl.ds(k * pair + c * rows, rows)] = coef_plane[c, dz, dy]
    second_pass(0, rows, ("anchor",))
    start(("r", 0), ("r", 1))
    second_pass(rows, 2 * rows, ("key", "anchor"))
    start(("r", 2), ("r", 3))
    arrived(("r", 0))
    total[pl.ds(KEY_POS[1] * rows, half), :] += relay[0]
    start(("r", 4))
    arrived(("r", 1))
    total[pl.ds(KEY_POS[3] * rows + half, half), :] += relay[1]
    start(("r", 5))
    losses = jnp.zeros((8, rows), F32)
    for cc in range(2):
        for zz in range(4):
            for yy in range(4):
                losses = losses + coef_plane[
                    lax.rem(cc + core, 2), lax.rem(zz + 4 - z, 4), lax.rem(yy + 4 - y, 4)
                ]
    loss_line[0] = losses
    start(*[("ox", d) for d in RING])
    second_pass(own_key, rows, ("key", "anchor"))

    arrived(*[("ox", d) for d in RING])
    sums = jnp.zeros((8, rows), F32)
    for xx in range(4):
        sums = sums + loss_line[lax.rem(xx + 4 - x, 4)]
    views = 128.0 * rows
    loss_ref[...] = jnp.broadcast_to(jnp.sum(sums, axis=1, keepdims=True), (8, rows)) / views

    arrived(("r", 2), ("r", 3), ("r", 4), ("r", 5))

    def finish(i, carry):
        here = pl.ds(pl.multiple_of(i * 16, 16), 16)
        there = pl.ds(pl.multiple_of(own_key + i * 16, 16), 16)
        values = student_ref[here, :].astype(F32)
        scaling = lax.rsqrt(jnp.sum(values * values, axis=1, keepdims=True) + epsilon)
        unit = values * scaling
        grad = total[there, :] + arrive[0, here, :] + arrive[1, here, :]
        along = jnp.sum(unit * grad, axis=1, keepdims=True)
        grad_ref[here, :] = scaling * (grad - unit * along)
        return carry

    lax.fori_loop(0, rows // 16, finish, 0)
    for name in NAMES:
        message(name).wait_send()


def body(student, teacher, labels):
    rows, width = student.shape
    keys, anchors = 4 * rows, 32 * rows
    vmem = pl.BlockSpec(memory_space=pltpu.VMEM)
    grad, losses = pl.pallas_call(
        kernel,
        out_shape=(
            jax.ShapeDtypeStruct((rows, width), F32),
            jax.ShapeDtypeStruct((8, rows), F32),
        ),
        in_specs=[vmem] * 3,
        out_specs=(vmem, vmem),
        scratch_shapes=[
            pltpu.VMEM((anchors, width), BF16),
            pltpu.VMEM((anchors, width), BF16),
            pltpu.VMEM((keys, width), BF16),
            pltpu.VMEM((keys, width), BF16),
            pltpu.VMEM((keys, 2 * rows), F32),
            pltpu.VMEM((keys, 2 * rows), F32),
            pltpu.VMEM((keys, anchors), F32),
            pltpu.VMEM((keys, anchors), F32),
            pltpu.VMEM((6, keys, rows), F32),
            pltpu.VMEM((keys, rows), F32),
            pltpu.VMEM((8, anchors), F32),
            pltpu.VMEM((2, 4, 4, 8, rows), F32),
            pltpu.VMEM((4, 8, rows), F32),
            pltpu.VMEM((4, 8, rows), F32),
            pltpu.VMEM((3, 4, 8, rows), F32),
            pltpu.VMEM((2, 4, 4, 8, rows), F32),
            pltpu.VMEM((4, keys, rows), F32),
            pltpu.VMEM((8, anchors), F32),
            pltpu.VMEM((4, 8, rows), F32),
            pltpu.VMEM((keys, 4 * rows), BF16),
            pltpu.VMEM((keys, 4 * rows), BF16),
            pltpu.VMEM((keys, width), F32),
            pltpu.VMEM((2, rows // 2, width), F32),
            pltpu.VMEM((2, rows, width), F32),
            pltpu.SemaphoreType.DMA((len(NAMES),)),
            pltpu.SemaphoreType.DMA((len(NAMES),)),
        ],
        compiler_params=pltpu.CompilerParams(
            collective_id=0, has_side_effects=True, vmem_limit_bytes=60 * 1024 * 1024
        ),
    )(student, teacher, labels.reshape(1, rows))
    return losses[4, 0], losses[5, 0], grad


def solution(mesh):
    torus = Mesh(mesh.devices.reshape(2, 2, 4, 2, 4), AXES)
    own = ("x_lo", "core", "z", "x_hi", "y")
    return jax.shard_map(
        body,
        mesh=torus,
        in_specs=(P(own, None), P(own, None), P(own)),
        out_specs=(P(), P(), P(own, None)),
        check_vma=False,
    )
```

```python
import math

import jax
import jax.numpy as jnp
from jax import lax
from jax.experimental import pallas as pl
from jax.experimental.pallas import tpu as pltpu
from jax.sharding import Mesh
from jax.sharding import PartitionSpec as P

AXES = ("x_lo", "core", "z", "x_hi", "y")
MESH = pl.DeviceIdType.MESH
F32, BF16 = jnp.float32, jnp.bfloat16

temp_sup = 0.1
temp_student = 0.2
temp_teacher = 0.05
epsilon = 1e-06
LOG2E = math.log2(math.e)

KEY_POS = {2: 0, 1: 1, 3: 2, 0: 3}
RING = (1, 2, 3)
OTHERS = [(dy, dz, c) for c in range(2) for dz in range(4) for dy in range(4)][1:]


def plane_messages():
    out = {}
    near = ((1, -1), (3, 1))

    def along(kind, axis, others):
        for d, step in near:
            for o in others:
                slot, source = ((d, o), (0, o)) if axis == "y" else ((o, d), (o, 0))
                for h in range(2):
                    out[kind, slot, h] = (source, axis, step)
        for o in others:
            for h, (d, step) in enumerate(near):
                slot, source = ((2, o), (d, o)) if axis == "y" else ((o, 2), (o, d))
                out[kind, slot, h] = (source, axis, step)

    along("u", "y", (0,))
    along("v", "z", (0,))
    along("u", "z", range(4))
    along("v", "y", range(4))
    return out


def line_messages():
    out = {}
    for kind in ("ku", "kv"):
        for d, step in ((1, -1), (3, 1)):
            for h in range(2):
                out[kind, d, h] = (0, "x", step)
        for h, (d, step) in enumerate(((1, -1), (3, 1))):
            out[kind, 2, h] = (d, "x", step)
    return out


MESSAGES = {**plane_messages(), **line_messages()}


PRIORITY = (
    62, 23, 50, 16, 52, 27, 0, 32, 58, 39, 6, 33, 66, 43, 60, 68, 13, 7,
    10, 56, 5, 49, 38, 18, 51, 54, 15, 1, 35, 46, 2, 55, 19, 29, 71, 44,
    64, 53, 59, 8, 37, 28, 67, 63, 70, 45, 47, 69, 17, 65, 3, 14, 30, 9,
    31, 36, 61, 4, 41, 11, 12, 48, 42, 22, 34, 40, 21, 24, 20, 25, 26, 57,
)


def make_schedule():
    wire, hop, tile, local = 2.8, 2.2, 1.4, 1.5
    order = dict(zip(MESSAGES, PRIORITY))
    free, arrive, waited, have = {}, {}, {}, {}

    def launch(name, when):
        _, axis, step = MESSAGES[name]
        free[axis, step] = max(free.get((axis, step), 0.0), when) + wire
        arrive[name] = free[axis, step] + hop

    def after(kind, slot, half):
        found = [
            n for n, m in MESSAGES.items() if n[0] == kind and m[0] == slot and n[2] == half
        ]
        return tuple(sorted(found, key=order.get))

    own = (("u", (0, 0)), ("v", (0, 0)), ("ku", 0), ("kv", 0))
    first = sorted((n for k in own for h in range(2) for n in after(*k, h)), key=order.get)
    for name in first:
        launch(name, 0.0)
    slots = [(dy, dz) for dz in range(4) for dy in range(4)]
    whole = {("u", (0, 0)): 0.0, ("v", (0, 0)): 0.0}
    now, tiles, steps, actions = 0.0, [], [], []
    lines = list(line_messages())

    def ready_at(slot):
        return max(whole.get((k, slot), 1e9) for k in ("u", "v")) + local

    while len(tiles) < 16:
        coming = min(((t, order[n], n) for n, t in arrive.items() if n not in waited), default=None)
        able = [s for s in slots if s not in tiles and ready_at(s) <= now]
        if not all(n in waited for n in lines):
            able = []
        if coming and (coming[0] <= now or not able):
            now = max(now, coming[0]) + 0.05
            name = coming[2]
            waited[name] = now
            follow = after(*name)
            for f in follow:
                launch(f, now)
            kind, slot, half = name
            complete = (kind, slot, 1 - half) in waited
            if complete:
                whole[kind, slot] = now
            actions.append((name, follow, complete and kind in ("u", "v")))
        elif able:
            best = min(able, key=lambda s: (ready_at(s), slots.index(s)))
            tiles.append(best)
            steps.append(tuple(actions))
            actions = []
            now += tile
        else:
            now = min(ready_at(s) for s in slots if s not in tiles) + 1e-6
    return tuple(first), tuple(steps), tuple(tiles), now


FIRST, STEPS, TILES, _ = make_schedule()
LATER = tuple(
    n
    for n in FIRST
    if MESSAGES[n][1] == "z" and n != next(m for m in FIRST if MESSAGES[m][1:] == MESSAGES[n][1:])
)
SLOT = {s: k for k, s in enumerate(TILES)}
NAMES = (
    list(MESSAGES)
    + [("pu", s) for s in TILES]
    + [("pv", s) for s in TILES]
    + [(kind, d) for kind in ("lx", "ly", "lz", "sx", "ox") for d in RING]
    + [("s", o) for o in OTHERS]
    + [("lp", 0)]
    + [("r", i) for i in range(6)]
)
IDS = {n: i for i, n in enumerate(NAMES)}


def kernel(
    student_hbm,
    teacher_hbm,
    label_ref,
    grad_ref,
    loss_ref,
    ua,
    va,
    uk,
    vk,
    raw_s,
    raw_t,
    signed_b,
    w_all,
    acc,
    key_label,
    anchor_label,
    label_plane,
    label_line,
    part,
    part_in,
    coef_plane,
    key_coef,
    anchor_coef,
    loss_line,
    gbuf0,
    gbuf1,
    total,
    relay,
    arrive,
    student_ref,
    teacher_ref,
    send_sem,
    recv_sem,
    load_sem,
):
    rows, width = student_ref.shape
    x_lo, x_hi = lax.axis_index("x_lo"), lax.axis_index("x_hi")
    core = lax.axis_index("core")
    y, z = lax.axis_index("y"), lax.axis_index("z")
    x = x_hi * 2 + x_lo
    pair = 2 * rows

    def device(axis, step):
        if axis == "core":
            return {"core": 1 - core}
        if axis == "x":
            there = lax.rem(x + step + 4, 4)
            return {"x_hi": there // 2, "x_lo": lax.rem(there, 2)}
        if axis == "plane":
            dy, dz, c = step
            there = {"y": lax.rem(y + 4 - dy, 4), "z": lax.rem(z + 4 - dz, 4)}
            return {**there, "core": 1 - core if c else core}
        place = y if axis == "y" else z
        return {axis: lax.rem(place + step + 4, 4)}

    def key_rows(d):
        return pl.ds(KEY_POS[d] * rows, rows)

    def own_rows(slot):
        return pl.ds(SLOT[slot] * pair, rows)

    half = rows // 2

    def part_of(start, h):
        return pl.ds(start + h * half, half)

    def refs_of(name):
        kind, slot = name[:2]
        if kind in ("u", "v"):
            source, axis, step = MESSAGES[name]
            buf = ua if kind == "u" else va
            here, there = SLOT[source] * pair, SLOT[slot] * pair
            return buf.at[part_of(here, name[2])], buf.at[part_of(there, name[2])], axis, step
        if kind in ("ku", "kv"):
            source, axis, step = MESSAGES[name]
            buf = uk if kind == "ku" else vk
            here, there = KEY_POS[source] * rows, KEY_POS[slot] * rows
            return buf.at[part_of(here, name[2])], buf.at[part_of(there, name[2])], axis, step
        if kind in ("pu", "pv"):
            buf = ua if kind == "pu" else va
            there = pl.ds(SLOT[slot] * pair + rows, rows)
            return buf.at[own_rows(slot)], buf.at[there], "core", 0
        if kind in ("lx", "ox"):
            buf = label_line if kind == "lx" else loss_line
            return buf.at[0], buf.at[slot], "x", -slot
        if kind == "sx":
            return part, part_in.at[slot - 1], "x", -slot
        if kind == "s":
            dy, dz, c = slot
            return coef_plane.at[0, 0, 0], coef_plane.at[c, dz, dy], "plane", slot
        if kind == "ly":
            return label_plane.at[0, 0, 0], label_plane.at[0, 0, slot], "y", -slot
        if kind == "lz":
            return label_plane.at[0, 0], label_plane.at[0, slot], "z", -slot
        if kind == "lp":
            return label_plane.at[0], label_plane.at[1], "core", 0
        two, nxt, prv = KEY_POS[2] * rows, KEY_POS[1] * rows, KEY_POS[3] * rows
        return (
            (total.at[pl.ds(two, half)], relay.at[0], "x", 1),
            (total.at[pl.ds(two + half, half)], relay.at[1], "x", -1),
            (total.at[pl.ds(nxt + half, half)], arrive.at[0, pl.ds(half, half)], "x", 1),
            (total.at[pl.ds(prv, half)], arrive.at[1, pl.ds(0, half)], "x", -1),
            (total.at[pl.ds(nxt, half)], arrive.at[0, pl.ds(0, half)], "x", 1),
            (total.at[pl.ds(prv + half, half)], arrive.at[1, pl.ds(half, half)], "x", -1),
        )[slot]

    def message(name):
        source, target, axis, step = refs_of(name)
        return pltpu.make_async_remote_copy(
            src_ref=source,
            dst_ref=target,
            send_sem=send_sem.at[IDS[name]],
            recv_sem=recv_sem.at[IDS[name]],
            device_id=device(axis, step),
            device_id_type=MESH,
        )

    def start(*names):
        for name in names:
            message(name).start()

    def arrived(*names):
        for name in names:
            message(name).wait_recv()

    loads = [
        pltpu.make_async_copy(student_hbm, student_ref, load_sem.at[0]),
        pltpu.make_async_copy(teacher_hbm, teacher_ref, load_sem.at[1]),
    ]
    for load in loads:
        load.start()

    barrier = pltpu.get_barrier_semaphore()
    for axis in ("x", "y", "z"):
        for d in RING:
            pl.semaphore_signal(barrier, inc=1, device_id=device(axis, d), device_id_type=MESH)
    pl.semaphore_signal(barrier, inc=1, device_id=device("core", 0), device_id_type=MESH)

    for load in loads:
        load.wait()
    own_key = KEY_POS[0] * rows

    def normalise(i, carry):
        here = pl.ds(pl.multiple_of(i * 16, 16), 16)
        there = pl.ds(pl.multiple_of(own_key + i * 16, 16), 16)
        for raw, anchors, keys in ((student_ref, ua, uk), (teacher_ref, va, vk)):
            values = raw[here, :].astype(F32)
            scaling = lax.rsqrt(jnp.sum(values * values, axis=1, keepdims=True) + epsilon)
            unit = (values * scaling).astype(BF16)
            anchors[here, :] = unit
            keys[there, :] = unit
        return carry

    lax.fori_loop(0, rows // 16, normalise, 0)
    own_label = jnp.broadcast_to(label_ref[...].astype(F32), (8, rows))
    label_plane[0, 0, 0] = own_label
    label_line[0] = own_label
    acc[...] = jnp.zeros_like(acc)
    total[...] = jnp.zeros_like(total)
    pl.semaphore_wait(barrier, 10)

    start(*[("ly", d) for d in RING], *[("lx", d) for d in RING])
    start(*[name for name in FIRST if name not in LATER])
    start(("pu", (0, 0)), ("pv", (0, 0)))
    arrived(*[("ly", d) for d in RING])
    start(*[("lz", d) for d in RING])
    start(*LATER)

    def labels_in():
        arrived(("lp", 0), *[("lx", d) for d in RING])
        for d in range(4):
            line = label_line[d][0:1]
            key_label[key_rows(d), :] = jnp.broadcast_to(line, (rows, rows)).T
        for (dy, dz), k in SLOT.items():
            for c in range(2):
                anchor_label[:, pl.ds(k * pair + c * rows, rows)] = label_plane[c, dz, dy]

    chunk = 32
    k_rel = LOG2E / temp_student
    k_tea = LOG2E / temp_teacher

    def elementwise(k, count, base, diagonal):
        def one(i, carry):
            r = pl.ds(pl.multiple_of(base + i * chunk, chunk), chunk)
            label = key_label[r, :]
            sums = [None] * 6
            for c in range(2):
                lanes = pl.ds(c * rows, rows)
                columns = pl.ds(pl.multiple_of(k * pair + c * rows, rows), rows)
                s = raw_s[r, lanes]
                t = raw_t[r, lanes]
                b = jnp.exp2(s * k_rel - k_rel)
                w = jnp.exp2(t * k_tea - k_tea)
                same = label == jnp.broadcast_to(anchor_label[0:1, columns], label.shape)
                if diagonal and c == 0:
                    row = lax.broadcasted_iota(jnp.int32, label.shape, 0) + i * chunk
                    lane = lax.broadcasted_iota(jnp.int32, label.shape, 1)
                    other = row != lane
                    same = jnp.logical_and(same, other)
                    b = jnp.where(other, b, 0.0)
                    w = jnp.where(other, w, 0.0)
                signed_b[r, columns] = jnp.where(same, -b, b)
                w_all[r, columns] = w
                values = (b * b, b, w, w * s, jnp.where(same, s, 0.0), jnp.where(same, 1.0, 0.0))
                sums = [v if p is None else p + v for p, v in zip(sums, values)]
            for n in range(6):
                acc[n, r, :] += sums[n]
            return carry

        lax.fori_loop(0, count // chunk, one, 0)

    key_count = 4 * rows
    contract = (((1,), (1,)), ((), ()))

    def tile_step(k, carry):
        for n, actions in enumerate(STEPS):
            @pl.when(k == n)
            def _(n=n, actions=actions):
                for i, (name, follow, complete) in enumerate(actions):
                    if n == 0 and i == 8:
                        arrived(*[("lz", d) for d in RING])
                        start(("lp", 0))
                    arrived(name)
                    start(*follow)
                    if complete:
                        start(("p" + name[0], name[1]))
                arrived(("pu", TILES[n]), ("pv", TILES[n]))
                if n == 0:
                    labels_in()

        here = pl.ds(pl.multiple_of(k * pair, pair), pair)
        raw_s[...] = lax.dot_general(uk[...], ua[here, :], contract, preferred_element_type=F32)
        raw_t[...] = lax.dot_general(vk[...], va[here, :], contract, preferred_element_type=F32)
        elementwise(k, key_count - rows, 0, False)

        @pl.when(k == 0)
        def _():
            elementwise(k, rows, own_key, True)

        @pl.when(k > 0)
        def _():
            elementwise(k, rows, own_key, False)

        return carry

    lax.fori_loop(0, 16, tile_step, 0)

    lane = lax.broadcasted_iota(jnp.int32, (rows, rows), 1)
    for d in range(4):
        packed = jnp.zeros((rows, rows), F32)
        for n in range(6):
            packed = jnp.where(
                lane == n, jnp.sum(acc[n, key_rows(d), :], axis=1, keepdims=True), packed
            )
        part[d] = packed.T[0:8]
    start(*[("sx", d) for d in RING])
    arrived(*[("sx", d) for d in RING])
    line = lax.broadcasted_iota(jnp.int32, (8, rows), 0)

    def coefficients(e):
        sums = part[e]
        for d in RING:
            sums = sums + part_in[d - 1, (e - d) % 4]
        sup, rel, tea = sums[0:1], sums[1:2], sums[2:3]
        positives = jnp.maximum(sums[5:6], 1.0)
        coefs = (
            (1.0 / temp_sup) / sup,
            (1.0 / temp_student) / rel,
            (1.0 / temp_student) / tea,
            (1.0 / temp_sup) / positives,
        )
        if e == 0:
            contrast = (1.0 - sums[4:5] / positives) / temp_sup + jnp.log(sup)
            relation = (1.0 - sums[3:4] / tea) / temp_student + jnp.log(rel)
            mine = jnp.zeros((8, rows), F32)
            for n, value in enumerate((*coefs, contrast, relation)):
                mine = jnp.where(line == n, jnp.broadcast_to(value, (8, rows)), mine)
            coef_plane[0, 0, 0] = mine
            start(*[("s", o) for o in OTHERS])
        for n in range(4):
            key_coef[n, key_rows(e), :] = jnp.broadcast_to(coefs[n], (rows, rows)).T

    depth = 4 * rows
    chunks = 32 * rows // depth

    def fill(c, ranges, sides, out):
        size = sum(count for _, count in ranges)
        blocks = [f + i for f, count in ranges for i in range(0, count, chunk)]
        for i, first in enumerate(blocks):
            r = pl.ds(first, chunk)
            for q in range(depth // rows):
                columns = pl.ds(pl.multiple_of(c * depth + q * rows, rows), rows)
                sb = signed_b[r, columns]
                w = w_all[r, columns]
                b, a, positive = jnp.abs(sb), sb * sb, sb < 0.0
                for n, side in enumerate(sides):
                    if side == "key":
                        ca, cb, cw, cp = [key_coef[m, r, :] for m in range(4)]
                    else:
                        ca, cb, cw, cp = [
                            jnp.broadcast_to(anchor_coef[m : m + 1, columns], sb.shape)
                            for m in range(4)
                        ]
                    value = (a * ca - jnp.where(positive, cp, 0.0)) + (b * cb - w * cw)
                    there = pl.ds(n * size + i * chunk, chunk)
                    out[there, pl.ds(q * rows, rows)] = value.astype(BF16)

    def multiply(c, ranges, sides, out):
        size = sum(count for _, count in ranges)
        anchors = ua[pl.ds(pl.multiple_of(c * depth, depth), depth), :]
        made = out[pl.ds(0, size * len(sides)), :]
        product = jnp.dot(made, anchors, preferred_element_type=F32)
        if len(sides) == 2:
            product = product[0:size] + product[size : 2 * size]
        at = 0
        for first, count in ranges:
            total[pl.ds(first, count), :] += product[at : at + count]
            at += count

    def coefficients_in(c):
        for k in range(c * depth // pair, (c + 1) * depth // pair):
            dy, dz = TILES[k]
            for side in range(2):
                if (dy, dz, side) != (0, 0, 0):
                    arrived(("s", (dy, dz, side)))
                anchor_coef[:, pl.ds(k * pair + side * rows, rows)] = coef_plane[side, dz, dy]

    def second_pass(ranges, sides, staged=False):
        if staged:
            coefficients_in(0)
        fill(0, ranges, sides, gbuf0)

        def one(j, carry):
            c = 2 * j
            if staged:
                for n in range(chunks // 2):
                    @pl.when(j == n)
                    def _(n=n):
                        for piece in range(2 * n + 1, min(2 * n + 3, chunks)):
                            coefficients_in(piece)

            multiply(c, ranges, sides, gbuf0)
            fill(c + 1, ranges, sides, gbuf1)
            multiply(c + 1, ranges, sides, gbuf1)
            fill(jnp.minimum(c + 2, chunks - 1), ranges, sides, gbuf0)
            return carry

        lax.fori_loop(0, chunks // 2, one, 0)

    both = ("key", "anchor")
    coefficients(0)
    coefficients(2)
    second_pass([(0, rows)], ("key",))
    coefficients(1)
    coefficients(3)
    second_pass([(0, rows)], ("anchor",), staged=True)
    start(("r", 0), ("r", 1))
    second_pass([(KEY_POS[1] * rows + half, rows)], both)
    start(("r", 2), ("r", 3))
    second_pass([(KEY_POS[1] * rows, half), (KEY_POS[3] * rows + half, half)], both)
    arrived(("r", 0))
    total[pl.ds(KEY_POS[1] * rows, half), :] += relay[0]
    start(("r", 4))
    arrived(("r", 1))
    total[pl.ds(KEY_POS[3] * rows + half, half), :] += relay[1]
    start(("r", 5))
    losses = jnp.zeros((8, rows), F32)
    for cc in range(2):
        for zz in range(4):
            for yy in range(4):
                losses = losses + coef_plane[
                    lax.rem(cc + core, 2), lax.rem(zz + 4 - z, 4), lax.rem(yy + 4 - y, 4)
                ]
    loss_line[0] = losses
    start(*[("ox", d) for d in RING])
    second_pass([(own_key, rows)], both)

    arrived(*[("ox", d) for d in RING])
    sums = jnp.zeros((8, rows), F32)
    for xx in range(4):
        sums = sums + loss_line[lax.rem(xx + 4 - x, 4)]
    views = 128.0 * rows
    loss_ref[...] = jnp.broadcast_to(jnp.sum(sums, axis=1, keepdims=True), (8, rows)) / views

    arrived(("r", 2), ("r", 3), ("r", 4), ("r", 5))

    def finish(i, carry):
        here = pl.ds(pl.multiple_of(i * 16, 16), 16)
        there = pl.ds(pl.multiple_of(own_key + i * 16, 16), 16)
        grad_ref[here, :] = total[there, :] + arrive[0, here, :] + arrive[1, here, :]
        return carry

    lax.fori_loop(0, rows // 16, finish, 0)
    for name in NAMES:
        message(name).wait_send()


def project(student_ref, sum_ref, loss_in_ref, grad_ref, supcon_ref, relation_ref):
    def one(i, carry):
        here = pl.ds(pl.multiple_of(i * 16, 16), 16)
        values = student_ref[here, :].astype(F32)
        scaling = lax.rsqrt(jnp.sum(values * values, axis=1, keepdims=True) + epsilon)
        unit = values * scaling
        grad = sum_ref[here, :]
        along = jnp.sum(unit * grad, axis=1, keepdims=True)
        grad_ref[here, :] = scaling * (grad - unit * along)
        return carry

    lax.fori_loop(0, student_ref.shape[0] // 16, one, 0)
    supcon_ref[0, 0] = loss_in_ref[4, 0]
    relation_ref[0, 0] = loss_in_ref[5, 0]


def body(student, teacher, labels):
    rows, width = student.shape
    keys, anchors = 4 * rows, 32 * rows
    vmem = pl.BlockSpec(memory_space=pltpu.VMEM)
    hbm = pl.BlockSpec(memory_space=pltpu.HBM)
    sums, losses = pl.pallas_call(
        kernel,
        out_shape=(
            jax.ShapeDtypeStruct((rows, width), F32),
            jax.ShapeDtypeStruct((8, rows), F32),
        ),
        in_specs=[hbm, hbm, vmem],
        out_specs=(vmem, vmem),
        scratch_shapes=[
            pltpu.VMEM((anchors, width), BF16),
            pltpu.VMEM((anchors, width), BF16),
            pltpu.VMEM((keys, width), BF16),
            pltpu.VMEM((keys, width), BF16),
            pltpu.VMEM((keys, 2 * rows), F32),
            pltpu.VMEM((keys, 2 * rows), F32),
            pltpu.VMEM((keys, anchors), F32),
            pltpu.VMEM((keys, anchors), F32),
            pltpu.VMEM((6, keys, rows), F32),
            pltpu.VMEM((keys, rows), F32),
            pltpu.VMEM((8, anchors), F32),
            pltpu.VMEM((2, 4, 4, 8, rows), F32),
            pltpu.VMEM((4, 8, rows), F32),
            pltpu.VMEM((4, 8, rows), F32),
            pltpu.VMEM((3, 4, 8, rows), F32),
            pltpu.VMEM((2, 4, 4, 8, rows), F32),
            pltpu.VMEM((4, keys, rows), F32),
            pltpu.VMEM((8, anchors), F32),
            pltpu.VMEM((4, 8, rows), F32),
            pltpu.VMEM((keys, 4 * rows), BF16),
            pltpu.VMEM((keys, 4 * rows), BF16),
            pltpu.VMEM((keys, width), F32),
            pltpu.VMEM((2, rows // 2, width), F32),
            pltpu.VMEM((2, rows, width), F32),
            pltpu.VMEM((rows, width), BF16),
            pltpu.VMEM((rows, width), BF16),
            pltpu.SemaphoreType.DMA((len(NAMES),)),
            pltpu.SemaphoreType.DMA((len(NAMES),)),
            pltpu.SemaphoreType.DMA((2,)),
        ],
        compiler_params=pltpu.CompilerParams(
            collective_id=0, has_side_effects=True, vmem_limit_bytes=60 * 1024 * 1024
        ),
    )(student, teacher, labels.reshape(1, rows))
    smem = pl.BlockSpec(memory_space=pltpu.SMEM)
    scalar = jax.ShapeDtypeStruct((1, 1), F32)
    grad, supcon, relation = pl.pallas_call(
        project,
        out_shape=(jax.ShapeDtypeStruct((rows, width), F32), scalar, scalar),
        in_specs=[vmem, vmem, smem],
        out_specs=(vmem, smem, smem),
    )(student, sums, losses)
    return supcon.reshape(()), relation.reshape(()), grad


def solution(mesh):
    torus = Mesh(mesh.devices.reshape(2, 2, 4, 2, 4), AXES)
    own = ("x_lo", "core", "z", "x_hi", "y")
    return jax.shard_map(
        body,
        mesh=torus,
        in_specs=(P(own, None), P(own, None), P(own)),
        out_specs=(P(), P(), P(own, None)),
        check_vma=False,
    )
```

```python
import math

import jax
import jax.numpy as jnp
from jax import lax
from jax.experimental import pallas as pl
from jax.experimental.pallas import tpu as pltpu
from jax.sharding import Mesh
from jax.sharding import PartitionSpec as P

AXES = ("x_lo", "core", "z", "x_hi", "y")
MESH = pl.DeviceIdType.MESH
F32, BF16 = jnp.float32, jnp.bfloat16

temp_sup = 0.1
temp_student = 0.2
temp_teacher = 0.05
epsilon = 1e-06
LOG2E = math.log2(math.e)

KEY_POS = {2: 0, 1: 1, 3: 2, 0: 3}
RING = (1, 2, 3)
OTHERS = [(dy, dz, c) for c in range(2) for dz in range(4) for dy in range(4)][1:]


def plane_messages():
    out = {}
    near = ((1, -1), (3, 1))

    def along(kind, axis, others):
        for d, step in near:
            for o in others:
                slot, source = ((d, o), (0, o)) if axis == "y" else ((o, d), (o, 0))
                for h in range(2):
                    out[kind, slot, h] = (source, axis, step)
        for o in others:
            for h, (d, step) in enumerate(near):
                slot, source = ((2, o), (d, o)) if axis == "y" else ((o, 2), (o, d))
                out[kind, slot, h] = (source, axis, step)

    along("u", "y", (0,))
    along("v", "z", (0,))
    along("u", "z", range(4))
    along("v", "y", range(4))
    return out


def line_messages():
    out = {}
    for kind in ("ku", "kv"):
        for d, step in ((1, -1), (3, 1)):
            for h in range(2):
                out[kind, d, h] = (0, "x", step)
        for h, (d, step) in enumerate(((1, -1), (3, 1))):
            out[kind, 2, h] = (d, "x", step)
    return out


MESSAGES = {**plane_messages(), **line_messages()}


PRIORITY = (
    62, 68, 46, 70, 12, 11, 71, 48, 31, 66, 13, 5, 35, 34, 4, 16, 19, 41,
    22, 25, 49, 54, 42, 32, 37, 6, 67, 56, 21, 40, 47, 55, 30, 8, 0, 63,
    61, 10, 24, 3, 1, 60, 18, 50, 28, 14, 2, 51, 29, 52, 64, 69, 17, 65,
    9, 53, 7, 43, 26, 20, 36, 23, 58, 38, 39, 44, 27, 45, 59, 33, 57, 15,
)


def make_schedule():
    wire, hop, tile, local = 2.82, 3.4, 1.3, 2.0
    order = dict(zip(MESSAGES, PRIORITY))
    free, arrive, waited, have = {}, {}, {}, {}

    def launch(name, when):
        _, axis, step = MESSAGES[name]
        free[axis, step] = max(free.get((axis, step), 0.0), when) + wire
        arrive[name] = free[axis, step] + hop

    def after(kind, slot, half):
        found = [
            n for n, m in MESSAGES.items() if n[0] == kind and m[0] == slot and n[2] == half
        ]
        return tuple(sorted(found, key=order.get))

    own = (("u", (0, 0)), ("v", (0, 0)), ("ku", 0), ("kv", 0))
    first = sorted((n for k in own for h in range(2) for n in after(*k, h)), key=order.get)
    for name in first:
        launch(name, 0.0)
    slots = [(dy, dz) for dz in range(4) for dy in range(4)]
    whole = {("u", (0, 0)): 0.0, ("v", (0, 0)): 0.0}
    now, tiles, steps, actions = 0.0, [], [], []
    lines = list(line_messages())

    def ready_at(slot):
        return max(whole.get((k, slot), 1e9) for k in ("u", "v")) + local

    while len(tiles) < 16:
        coming = min(((t, order[n], n) for n, t in arrive.items() if n not in waited), default=None)
        able = [s for s in slots if s not in tiles and ready_at(s) <= now]
        if not all(n in waited for n in lines):
            able = []
        if coming and (coming[0] <= now or not able):
            now = max(now, coming[0]) + 0.05
            name = coming[2]
            waited[name] = now
            follow = after(*name)
            for f in follow:
                launch(f, now)
            kind, slot, half = name
            complete = (kind, slot, 1 - half) in waited
            if complete:
                whole[kind, slot] = now
            actions.append((name, follow, complete and kind in ("u", "v")))
        elif able:
            best = min(able, key=lambda s: (ready_at(s), slots.index(s)))
            tiles.append(best)
            steps.append(tuple(actions))
            actions = []
            now += tile
        else:
            now = min(ready_at(s) for s in slots if s not in tiles) + 1e-6
    return tuple(first), tuple(steps), tuple(tiles), now


FIRST, STEPS, TILES, _ = make_schedule()
LATER = tuple(
    n
    for n in FIRST
    if MESSAGES[n][1] == "z" and n != next(m for m in FIRST if MESSAGES[m][1:] == MESSAGES[n][1:])
)
SLOT = {s: k for k, s in enumerate(TILES)}
NAMES = (
    list(MESSAGES)
    + [("pu", s) for s in TILES]
    + [("pv", s) for s in TILES]
    + [(kind, d) for kind in ("lx", "ly", "lz", "sx", "ox") for d in RING]
    + [("s", o) for o in OTHERS]
    + [("lp", 0)]
    + [("r", i) for i in range(6)]
)
IDS = {n: i for i, n in enumerate(NAMES)}


def kernel(
    student_hbm,
    teacher_hbm,
    label_ref,
    sum_hbm,
    loss_ref,
    ua,
    va,
    uk,
    vk,
    raw_s,
    raw_t,
    signed_b,
    w_all,
    acc,
    key_label,
    anchor_label,
    label_plane,
    label_line,
    part,
    part_in,
    coef_plane,
    key_coef,
    anchor_coef,
    loss_line,
    gbuf0,
    gbuf1,
    total,
    relay,
    arrive,
    student_ref,
    teacher_ref,
    send_sem,
    recv_sem,
    load_sem,
):
    rows, width = student_ref.shape
    x_lo, x_hi = lax.axis_index("x_lo"), lax.axis_index("x_hi")
    core = lax.axis_index("core")
    y, z = lax.axis_index("y"), lax.axis_index("z")
    x = x_hi * 2 + x_lo
    pair = 2 * rows

    def device(axis, step):
        if axis == "core":
            return {"core": 1 - core}
        if axis == "x":
            there = lax.rem(x + step + 4, 4)
            return {"x_hi": there // 2, "x_lo": lax.rem(there, 2)}
        if axis == "plane":
            dy, dz, c = step
            there = {"y": lax.rem(y + 4 - dy, 4), "z": lax.rem(z + 4 - dz, 4)}
            return {**there, "core": 1 - core if c else core}
        place = y if axis == "y" else z
        return {axis: lax.rem(place + step + 4, 4)}

    def key_rows(d):
        return pl.ds(KEY_POS[d] * rows, rows)

    def own_rows(slot):
        return pl.ds(SLOT[slot] * pair, rows)

    half = rows // 2

    def part_of(start, h):
        return pl.ds(start + h * half, half)

    def refs_of(name):
        kind, slot = name[:2]
        if kind in ("u", "v"):
            source, axis, step = MESSAGES[name]
            buf = ua if kind == "u" else va
            here, there = SLOT[source] * pair, SLOT[slot] * pair
            return buf.at[part_of(here, name[2])], buf.at[part_of(there, name[2])], axis, step
        if kind in ("ku", "kv"):
            source, axis, step = MESSAGES[name]
            buf = uk if kind == "ku" else vk
            here, there = KEY_POS[source] * rows, KEY_POS[slot] * rows
            return buf.at[part_of(here, name[2])], buf.at[part_of(there, name[2])], axis, step
        if kind in ("pu", "pv"):
            buf = ua if kind == "pu" else va
            there = pl.ds(SLOT[slot] * pair + rows, rows)
            return buf.at[own_rows(slot)], buf.at[there], "core", 0
        if kind in ("lx", "ox"):
            buf = label_line if kind == "lx" else loss_line
            return buf.at[0], buf.at[slot], "x", -slot
        if kind == "sx":
            return part, part_in.at[slot - 1], "x", -slot
        if kind == "s":
            dy, dz, c = slot
            return coef_plane.at[0, 0, 0], coef_plane.at[c, dz, dy], "plane", slot
        if kind == "ly":
            return label_plane.at[0, 0, 0], label_plane.at[0, 0, slot], "y", -slot
        if kind == "lz":
            return label_plane.at[0, 0], label_plane.at[0, slot], "z", -slot
        if kind == "lp":
            return label_plane.at[0], label_plane.at[1], "core", 0
        two, nxt, prv = KEY_POS[2] * rows, KEY_POS[1] * rows, KEY_POS[3] * rows
        return (
            (total.at[pl.ds(two, half)], relay.at[0], "x", 1),
            (total.at[pl.ds(two + half, half)], relay.at[1], "x", -1),
            (total.at[pl.ds(nxt + half, half)], arrive.at[0, pl.ds(half, half)], "x", 1),
            (total.at[pl.ds(prv, half)], arrive.at[1, pl.ds(0, half)], "x", -1),
            (total.at[pl.ds(nxt, half)], arrive.at[0, pl.ds(0, half)], "x", 1),
            (total.at[pl.ds(prv + half, half)], arrive.at[1, pl.ds(half, half)], "x", -1),
        )[slot]

    def message(name):
        source, target, axis, step = refs_of(name)
        return pltpu.make_async_remote_copy(
            src_ref=source,
            dst_ref=target,
            send_sem=send_sem.at[IDS[name]],
            recv_sem=recv_sem.at[IDS[name]],
            device_id=device(axis, step),
            device_id_type=MESH,
        )

    def start(*names):
        for name in names:
            message(name).start()

    def arrived(*names):
        for name in names:
            message(name).wait_recv()

    loads = [
        pltpu.make_async_copy(student_hbm, student_ref, load_sem.at[0]),
        pltpu.make_async_copy(teacher_hbm, teacher_ref, load_sem.at[1]),
    ]
    for load in loads:
        load.start()

    barrier = pltpu.get_barrier_semaphore()
    for axis in ("x", "y", "z"):
        for d in RING:
            pl.semaphore_signal(barrier, inc=1, device_id=device(axis, d), device_id_type=MESH)
    pl.semaphore_signal(barrier, inc=1, device_id=device("core", 0), device_id_type=MESH)

    for load in loads:
        load.wait()
    own_key = KEY_POS[0] * rows

    def normalise(i, carry):
        here = pl.ds(pl.multiple_of(i * 16, 16), 16)
        there = pl.ds(pl.multiple_of(own_key + i * 16, 16), 16)
        for raw, anchors, keys in ((student_ref, ua, uk), (teacher_ref, va, vk)):
            values = raw[here, :].astype(F32)
            scaling = lax.rsqrt(jnp.sum(values * values, axis=1, keepdims=True) + epsilon)
            unit = (values * scaling).astype(BF16)
            anchors[here, :] = unit
            keys[there, :] = unit
        return carry

    lax.fori_loop(0, rows // 16, normalise, 0, unroll=4)
    own_label = jnp.broadcast_to(label_ref[...].astype(F32), (8, rows))
    label_plane[0, 0, 0] = own_label
    label_line[0] = own_label
    pl.semaphore_wait(barrier, 10)

    start(*[("ly", d) for d in RING], *[("lx", d) for d in RING])
    start(*[name for name in FIRST if name not in LATER])
    start(("pu", (0, 0)), ("pv", (0, 0)))
    acc[...] = jnp.zeros_like(acc)
    total[...] = jnp.zeros_like(total)
    arrived(*[("ly", d) for d in RING])
    start(*[("lz", d) for d in RING])
    start(*LATER)

    def labels_in():
        arrived(("lp", 0), *[("lx", d) for d in RING])
        for d in range(4):
            line = label_line[d][0:1]
            key_label[key_rows(d), :] = jnp.broadcast_to(line, (rows, rows)).T
        for (dy, dz), k in SLOT.items():
            for c in range(2):
                anchor_label[:, pl.ds(k * pair + c * rows, rows)] = label_plane[c, dz, dy]

    chunk = 32
    k_rel = LOG2E / temp_student
    k_tea = LOG2E / temp_teacher

    def elementwise(k, count, base, diagonal):
        def one(i, carry):
            r = pl.ds(pl.multiple_of(base + i * chunk, chunk), chunk)
            label = key_label[r, :]
            sums = [None] * 6
            for c in range(2):
                lanes = pl.ds(c * rows, rows)
                columns = pl.ds(pl.multiple_of(k * pair + c * rows, rows), rows)
                s = raw_s[r, lanes]
                t = raw_t[r, lanes]
                b = jnp.exp2(s * k_rel - k_rel)
                w = jnp.exp2(t * k_tea - k_tea)
                same = label == jnp.broadcast_to(anchor_label[0:1, columns], label.shape)
                if diagonal and c == 0:
                    row = lax.broadcasted_iota(jnp.int32, label.shape, 0) + i * chunk
                    lane = lax.broadcasted_iota(jnp.int32, label.shape, 1)
                    other = row != lane
                    same = jnp.logical_and(same, other)
                    b = jnp.where(other, b, 0.0)
                    w = jnp.where(other, w, 0.0)
                signed_b[r, columns] = jnp.where(same, -b, b)
                w_all[r, columns] = w
                values = (b * b, b, w, w * s, jnp.where(same, s, 0.0), jnp.where(same, 1.0, 0.0))
                sums = [v if p is None else p + v for p, v in zip(sums, values)]
            for n in range(6):
                acc[n, r, :] += sums[n]
            return carry

        lax.fori_loop(0, count // chunk, one, 0)

    key_count = 4 * rows
    contract = (((1,), (1,)), ((), ()))

    def tile_step(k, carry):
        for n, actions in enumerate(STEPS):
            @pl.when(k == n)
            def _(n=n, actions=actions):
                for i, (name, follow, complete) in enumerate(actions):
                    if n == 0 and i == 8:
                        arrived(*[("lz", d) for d in RING])
                        start(("lp", 0))
                    arrived(name)
                    start(*follow)
                    if complete:
                        start(("p" + name[0], name[1]))
                arrived(("pu", TILES[n]), ("pv", TILES[n]))
                if n == 0:
                    labels_in()

        here = pl.ds(pl.multiple_of(k * pair, pair), pair)
        raw_s[...] = lax.dot_general(uk[...], ua[here, :], contract, preferred_element_type=F32)
        raw_t[...] = lax.dot_general(vk[...], va[here, :], contract, preferred_element_type=F32)
        elementwise(k, key_count - rows, 0, False)

        @pl.when(k == 0)
        def _():
            elementwise(k, rows, own_key, True)

        @pl.when(k > 0)
        def _():
            elementwise(k, rows, own_key, False)

        return carry

    lax.fori_loop(0, 16, tile_step, 0)

    lane = lax.broadcasted_iota(jnp.int32, (rows, rows), 1)
    for d in range(4):
        packed = jnp.zeros((rows, rows), F32)
        for n in range(6):
            packed = jnp.where(
                lane == n, jnp.sum(acc[n, key_rows(d), :], axis=1, keepdims=True), packed
            )
        part[d] = packed.T[0:8]
    start(*[("sx", d) for d in RING])
    arrived(*[("sx", d) for d in RING])
    line = lax.broadcasted_iota(jnp.int32, (8, rows), 0)

    def coefficients(e):
        sums = part[e]
        for d in RING:
            sums = sums + part_in[d - 1, (e - d) % 4]
        sup, rel, tea = sums[0:1], sums[1:2], sums[2:3]
        positives = jnp.maximum(sums[5:6], 1.0)
        coefs = (
            (1.0 / temp_sup) / sup,
            (1.0 / temp_student) / rel,
            (1.0 / temp_student) / tea,
            (1.0 / temp_sup) / positives,
        )
        if e == 0:
            contrast = (1.0 - sums[4:5] / positives) / temp_sup + jnp.log(sup)
            relation = (1.0 - sums[3:4] / tea) / temp_student + jnp.log(rel)
            mine = jnp.zeros((8, rows), F32)
            for n, value in enumerate((*coefs, contrast, relation)):
                mine = jnp.where(line == n, jnp.broadcast_to(value, (8, rows)), mine)
            coef_plane[0, 0, 0] = mine
            start(*[("s", o) for o in OTHERS])
        for n in range(4):
            key_coef[n, key_rows(e), :] = jnp.broadcast_to(coefs[n], (rows, rows)).T

    depth = 4 * rows
    chunks = 32 * rows // depth

    def fill(c, ranges, sides, out):
        size = sum(count for _, count in ranges)
        blocks = [f + i for f, count in ranges for i in range(0, count, chunk)]
        for i, first in enumerate(blocks):
            r = pl.ds(first, chunk)
            for q in range(depth // rows):
                columns = pl.ds(pl.multiple_of(c * depth + q * rows, rows), rows)
                sb = signed_b[r, columns]
                w = w_all[r, columns]
                b, a, positive = jnp.abs(sb), sb * sb, sb < 0.0
                for n, side in enumerate(sides):
                    if side == "key":
                        ca, cb, cw, cp = [key_coef[m, r, :] for m in range(4)]
                    else:
                        ca, cb, cw, cp = [
                            jnp.broadcast_to(anchor_coef[m : m + 1, columns], sb.shape)
                            for m in range(4)
                        ]
                    value = (a * ca - jnp.where(positive, cp, 0.0)) + (b * cb - w * cw)
                    there = pl.ds(n * size + i * chunk, chunk)
                    out[there, pl.ds(q * rows, rows)] = value.astype(BF16)

    def multiply(c, ranges, sides, out):
        size = sum(count for _, count in ranges)
        anchors = ua[pl.ds(pl.multiple_of(c * depth, depth), depth), :]
        made = out[pl.ds(0, size * len(sides)), :]
        product = jnp.dot(made, anchors, preferred_element_type=F32)
        if len(sides) == 2:
            product = product[0:size] + product[size : 2 * size]
        at = 0
        for first, count in ranges:
            total[pl.ds(first, count), :] += product[at : at + count]
            at += count

    def coefficients_in(c):
        for k in range(c * depth // pair, (c + 1) * depth // pair):
            dy, dz = TILES[k]
            for side in range(2):
                if (dy, dz, side) != (0, 0, 0):
                    arrived(("s", (dy, dz, side)))
                anchor_coef[:, pl.ds(k * pair + side * rows, rows)] = coef_plane[side, dz, dy]

    def second_pass(ranges, sides, staged=False):
        if staged:
            coefficients_in(0)
        fill(0, ranges, sides, gbuf0)

        def one(j, carry):
            c = 2 * j
            if staged:
                for n in range(chunks // 2):
                    @pl.when(j == n)
                    def _(n=n):
                        for piece in range(2 * n + 1, min(2 * n + 3, chunks)):
                            coefficients_in(piece)

            multiply(c, ranges, sides, gbuf0)
            fill(c + 1, ranges, sides, gbuf1)
            multiply(c + 1, ranges, sides, gbuf1)
            fill(jnp.minimum(c + 2, chunks - 1), ranges, sides, gbuf0)
            return carry

        lax.fori_loop(0, chunks // 2, one, 0)

    both = ("key", "anchor")
    coefficients(0)
    coefficients(2)
    second_pass([(0, rows)], ("key",))
    coefficients(1)
    coefficients(3)
    second_pass([(0, rows)], ("anchor",), staged=True)
    start(("r", 0), ("r", 1))
    second_pass([(KEY_POS[1] * rows + half, rows)], both)
    start(("r", 2), ("r", 3))
    second_pass([(KEY_POS[1] * rows, half), (KEY_POS[3] * rows + half, half)], both)
    arrived(("r", 0))
    total[pl.ds(KEY_POS[1] * rows, half), :] += relay[0]
    start(("r", 4))
    arrived(("r", 1))
    total[pl.ds(KEY_POS[3] * rows + half, half), :] += relay[1]
    start(("r", 5))
    losses = jnp.zeros((8, rows), F32)
    for cc in range(2):
        for zz in range(4):
            for yy in range(4):
                losses = losses + coef_plane[
                    lax.rem(cc + core, 2), lax.rem(zz + 4 - z, 4), lax.rem(yy + 4 - y, 4)
                ]
    loss_line[0] = losses
    start(*[("ox", d) for d in RING])
    second_pass([(own_key, rows)], both)

    arrived(*[("ox", d) for d in RING])
    sums = jnp.zeros((8, rows), F32)
    for xx in range(4):
        sums = sums + loss_line[lax.rem(xx + 4 - x, 4)]
    views = 128.0 * rows
    loss_ref[...] = jnp.broadcast_to(jnp.sum(sums, axis=1, keepdims=True), (8, rows)) / views

    arrived(("r", 2), ("r", 3), ("r", 4), ("r", 5))

    piece = rows // 4
    stores = []
    for i in range(4):
        here = pl.ds(i * piece, piece)
        mine = pl.ds(own_key + i * piece, piece)
        total[mine, :] += arrive[0, here, :] + arrive[1, here, :]
        store = pltpu.make_async_copy(total.at[mine], sum_hbm.at[here], load_sem.at[2 + i])
        store.start()
        stores.append(store)
    for store in stores:
        store.wait()
    for name in NAMES:
        message(name).wait_send()


def project(
    student_hbm,
    sum_hbm,
    loss_hbm,
    grad_hbm,
    supcon_ref,
    relation_ref,
    student_ref,
    sum_ref,
    loss_ref,
    grad_ref,
    load_sem,
    store_sem,
):
    rows = student_ref.shape[0]
    piece = 32
    pieces = [pl.ds(i, piece) for i in range(0, rows, piece)]
    loads = []
    for i, here in enumerate(pieces):
        loads.append(
            (
                pltpu.make_async_copy(sum_hbm.at[here], sum_ref.at[here], load_sem.at[0, i]),
                pltpu.make_async_copy(
                    student_hbm.at[here], student_ref.at[here], load_sem.at[1, i]
                ),
            )
        )
    loss_load = pltpu.make_async_copy(loss_hbm, loss_ref, load_sem.at[2, 0])
    for pair in loads:
        for load in pair:
            load.start()
    loss_load.start()
    stores = []
    for i, here in enumerate(pieces):
        for load in loads[i]:
            load.wait()
        for r in range(0, piece, 16):
            part = pl.ds(i * piece + r, 16)
            values = student_ref[part, :].astype(F32)
            scaling = lax.rsqrt(jnp.sum(values * values, axis=1, keepdims=True) + epsilon)
            unit = values * scaling
            grad = sum_ref[part, :]
            along = jnp.sum(unit * grad, axis=1, keepdims=True)
            grad_ref[part, :] = scaling * (grad - unit * along)
        store = pltpu.make_async_copy(grad_ref.at[here], grad_hbm.at[here], store_sem.at[i])
        store.start()
        stores.append(store)
    loss_load.wait()
    supcon_ref[0, 0] = loss_ref[4, 0]
    relation_ref[0, 0] = loss_ref[5, 0]
    for store in stores:
        store.wait()


def body(student, teacher, labels):
    rows, width = student.shape
    keys, anchors = 4 * rows, 32 * rows
    vmem = pl.BlockSpec(memory_space=pltpu.VMEM)
    hbm = pl.BlockSpec(memory_space=pltpu.HBM)
    sums, losses = pl.pallas_call(
        kernel,
        out_shape=(
            jax.ShapeDtypeStruct((rows, width), F32),
            jax.ShapeDtypeStruct((8, rows), F32),
        ),
        in_specs=[hbm, hbm, vmem],
        out_specs=(hbm, vmem),
        scratch_shapes=[
            pltpu.VMEM((anchors, width), BF16),
            pltpu.VMEM((anchors, width), BF16),
            pltpu.VMEM((keys, width), BF16),
            pltpu.VMEM((keys, width), BF16),
            pltpu.VMEM((keys, 2 * rows), F32),
            pltpu.VMEM((keys, 2 * rows), F32),
            pltpu.VMEM((keys, anchors), F32),
            pltpu.VMEM((keys, anchors), F32),
            pltpu.VMEM((6, keys, rows), F32),
            pltpu.VMEM((keys, rows), F32),
            pltpu.VMEM((8, anchors), F32),
            pltpu.VMEM((2, 4, 4, 8, rows), F32),
            pltpu.VMEM((4, 8, rows), F32),
            pltpu.VMEM((4, 8, rows), F32),
            pltpu.VMEM((3, 4, 8, rows), F32),
            pltpu.VMEM((2, 4, 4, 8, rows), F32),
            pltpu.VMEM((4, keys, rows), F32),
            pltpu.VMEM((8, anchors), F32),
            pltpu.VMEM((4, 8, rows), F32),
            pltpu.VMEM((keys, 4 * rows), BF16),
            pltpu.VMEM((keys, 4 * rows), BF16),
            pltpu.VMEM((keys, width), F32),
            pltpu.VMEM((2, rows // 2, width), F32),
            pltpu.VMEM((2, rows, width), F32),
            pltpu.VMEM((rows, width), BF16),
            pltpu.VMEM((rows, width), BF16),
            pltpu.SemaphoreType.DMA((len(NAMES),)),
            pltpu.SemaphoreType.DMA((len(NAMES),)),
            pltpu.SemaphoreType.DMA((6,)),
        ],
        compiler_params=pltpu.CompilerParams(
            collective_id=0, has_side_effects=True, vmem_limit_bytes=60 * 1024 * 1024
        ),
    )(student, teacher, labels.reshape(1, rows))
    smem = pl.BlockSpec(memory_space=pltpu.SMEM)
    scalar = jax.ShapeDtypeStruct((1, 1), F32)
    grad, supcon, relation = pl.pallas_call(
        project,
        out_shape=(jax.ShapeDtypeStruct((rows, width), F32), scalar, scalar),
        in_specs=[hbm, hbm, hbm],
        out_specs=(hbm, smem, smem),
        scratch_shapes=[
            pltpu.VMEM((rows, width), BF16),
            pltpu.VMEM((rows, width), F32),
            pltpu.SMEM((8, rows), F32),
            pltpu.VMEM((rows, width), F32),
            pltpu.SemaphoreType.DMA((3, rows // 32)),
            pltpu.SemaphoreType.DMA((rows // 32,)),
        ],
    )(student, sums, losses)
    return supcon.reshape(()), relation.reshape(()), grad


def solution(mesh):
    torus = Mesh(mesh.devices.reshape(2, 2, 4, 2, 4), AXES)
    own = ("x_lo", "core", "z", "x_hi", "y")
    return jax.shard_map(
        body,
        mesh=torus,
        in_specs=(P(own, None), P(own, None), P(own)),
        out_specs=(P(), P(), P(own, None)),
        check_vma=False,
    )
```

```python
import math

import jax
import jax.numpy as jnp
from jax import lax
from jax.experimental import pallas as pl
from jax.experimental.pallas import tpu as pltpu
from jax.sharding import Mesh
from jax.sharding import PartitionSpec as P

AXES = ("x_lo", "core", "z", "x_hi", "y")
MESH = pl.DeviceIdType.MESH
F32, BF16 = jnp.float32, jnp.bfloat16

temp_sup = 0.1
temp_student = 0.2
temp_teacher = 0.05
epsilon = 1e-06
LOG2E = math.log2(math.e)

KEY_POS = {2: 0, 1: 1, 3: 2, 0: 3}
RING = (1, 2, 3)
OTHERS = [(dy, dz, c) for c in range(2) for dz in range(4) for dy in range(4)][1:]


def plane_messages():
    out = {}
    near = ((1, -1), (3, 1))

    def along(kind, axis, others):
        for d, step in near:
            for o in others:
                slot, source = ((d, o), (0, o)) if axis == "y" else ((o, d), (o, 0))
                for h in range(2):
                    out[kind, slot, h] = (source, axis, step)
        for o in others:
            for h, (d, step) in enumerate(near):
                slot, source = ((2, o), (d, o)) if axis == "y" else ((o, 2), (o, d))
                out[kind, slot, h] = (source, axis, step)

    along("u", "y", (0,))
    along("v", "z", (0,))
    along("u", "z", range(4))
    along("v", "y", range(4))
    return out


def line_messages():
    out = {}
    for kind in ("ku", "kv"):
        for d, step in ((1, -1), (3, 1)):
            for h in range(2):
                out[kind, d, h] = (0, "x", step)
        for h, (d, step) in enumerate(((1, -1), (3, 1))):
            out[kind, 2, h] = (d, "x", step)
    return out


MESSAGES = {**plane_messages(), **line_messages()}


PRIORITY = (
    62, 68, 46, 70, 12, 11, 71, 48, 31, 66, 13, 5, 35, 34, 4, 16, 19, 41,
    22, 25, 49, 54, 42, 32, 37, 6, 67, 56, 21, 40, 47, 55, 30, 8, 0, 63,
    61, 10, 24, 3, 1, 60, 18, 50, 28, 14, 2, 51, 29, 52, 64, 69, 17, 65,
    9, 53, 7, 43, 26, 20, 36, 23, 58, 38, 39, 44, 27, 45, 59, 33, 57, 15,
)


def make_schedule():
    wire, hop, tile, local = 2.82, 3.4, 1.3, 2.0
    order = dict(zip(MESSAGES, PRIORITY))
    free, arrive, waited, have = {}, {}, {}, {}

    def launch(name, when):
        _, axis, step = MESSAGES[name]
        free[axis, step] = max(free.get((axis, step), 0.0), when) + wire
        arrive[name] = free[axis, step] + hop

    def after(kind, slot, half):
        found = [
            n for n, m in MESSAGES.items() if n[0] == kind and m[0] == slot and n[2] == half
        ]
        return tuple(sorted(found, key=order.get))

    own = (("u", (0, 0)), ("v", (0, 0)), ("ku", 0), ("kv", 0))
    first = sorted((n for k in own for h in range(2) for n in after(*k, h)), key=order.get)
    for name in first:
        launch(name, 0.0)
    slots = [(dy, dz) for dz in range(4) for dy in range(4)]
    whole = {("u", (0, 0)): 0.0, ("v", (0, 0)): 0.0}
    now, tiles, steps, actions = 0.0, [], [], []
    lines = list(line_messages())

    def ready_at(slot):
        return max(whole.get((k, slot), 1e9) for k in ("u", "v")) + local

    while len(tiles) < 16:
        coming = min(((t, order[n], n) for n, t in arrive.items() if n not in waited), default=None)
        able = [s for s in slots if s not in tiles and ready_at(s) <= now]
        if not all(n in waited for n in lines):
            able = []
        if coming and (coming[0] <= now or not able):
            now = max(now, coming[0]) + 0.05
            name = coming[2]
            waited[name] = now
            follow = after(*name)
            for f in follow:
                launch(f, now)
            kind, slot, half = name
            complete = (kind, slot, 1 - half) in waited
            if complete:
                whole[kind, slot] = now
            actions.append((name, follow, complete and kind in ("u", "v")))
        elif able:
            best = min(able, key=lambda s: (ready_at(s), slots.index(s)))
            tiles.append(best)
            steps.append(tuple(actions))
            actions = []
            now += tile
        else:
            now = min(ready_at(s) for s in slots if s not in tiles) + 1e-6
    return tuple(first), tuple(steps), tuple(tiles), now


FIRST, STEPS, TILES, _ = make_schedule()
LATER = tuple(
    n
    for n in FIRST
    if MESSAGES[n][1] == "z" and n != next(m for m in FIRST if MESSAGES[m][1:] == MESSAGES[n][1:])
)
SLOT = {s: k for k, s in enumerate(TILES)}
NAMES = (
    list(MESSAGES)
    + [("pu", s) for s in TILES]
    + [("pv", s) for s in TILES]
    + [(kind, d) for kind in ("lx", "ly", "lz", "sx", "ox") for d in RING]
    + [("s", o) for o in OTHERS]
    + [("lp", 0)]
    + [("r", i) for i in range(6)]
)
IDS = {n: i for i, n in enumerate(NAMES)}


def kernel(
    student_hbm,
    teacher_hbm,
    label_ref,
    grad_ref,
    loss_ref,
    ua,
    va,
    uk,
    vk,
    raw_s,
    raw_t,
    signed_b,
    w_all,
    acc,
    key_label,
    anchor_label,
    label_plane,
    label_line,
    part,
    part_in,
    coef_plane,
    key_coef,
    anchor_coef,
    loss_line,
    gbuf0,
    gbuf1,
    total,
    relay,
    arrive,
    student_ref,
    teacher_ref,
    send_sem,
    recv_sem,
    load_sem,
):
    rows, width = student_ref.shape
    x_lo, x_hi = lax.axis_index("x_lo"), lax.axis_index("x_hi")
    core = lax.axis_index("core")
    y, z = lax.axis_index("y"), lax.axis_index("z")
    x = x_hi * 2 + x_lo
    pair = 2 * rows

    def device(axis, step):
        if axis == "core":
            return {"core": 1 - core}
        if axis == "x":
            there = lax.rem(x + step + 4, 4)
            return {"x_hi": there // 2, "x_lo": lax.rem(there, 2)}
        if axis == "plane":
            dy, dz, c = step
            there = {"y": lax.rem(y + 4 - dy, 4), "z": lax.rem(z + 4 - dz, 4)}
            return {**there, "core": 1 - core if c else core}
        place = y if axis == "y" else z
        return {axis: lax.rem(place + step + 4, 4)}

    def key_rows(d):
        return pl.ds(KEY_POS[d] * rows, rows)

    def own_rows(slot):
        return pl.ds(SLOT[slot] * pair, rows)

    half = rows // 2

    def part_of(start, h):
        return pl.ds(start + h * half, half)

    def refs_of(name):
        kind, slot = name[:2]
        if kind in ("u", "v"):
            source, axis, step = MESSAGES[name]
            buf = ua if kind == "u" else va
            here, there = SLOT[source] * pair, SLOT[slot] * pair
            return buf.at[part_of(here, name[2])], buf.at[part_of(there, name[2])], axis, step
        if kind in ("ku", "kv"):
            source, axis, step = MESSAGES[name]
            buf = uk if kind == "ku" else vk
            here, there = KEY_POS[source] * rows, KEY_POS[slot] * rows
            return buf.at[part_of(here, name[2])], buf.at[part_of(there, name[2])], axis, step
        if kind in ("pu", "pv"):
            buf = ua if kind == "pu" else va
            there = pl.ds(SLOT[slot] * pair + rows, rows)
            return buf.at[own_rows(slot)], buf.at[there], "core", 0
        if kind in ("lx", "ox"):
            buf = label_line if kind == "lx" else loss_line
            return buf.at[0], buf.at[slot], "x", -slot
        if kind == "sx":
            return part, part_in.at[slot - 1], "x", -slot
        if kind == "s":
            dy, dz, c = slot
            return coef_plane.at[0, 0, 0], coef_plane.at[c, dz, dy], "plane", slot
        if kind == "ly":
            return label_plane.at[0, 0, 0], label_plane.at[0, 0, slot], "y", -slot
        if kind == "lz":
            return label_plane.at[0, 0], label_plane.at[0, slot], "z", -slot
        if kind == "lp":
            return label_plane.at[0], label_plane.at[1], "core", 0
        two, nxt, prv = KEY_POS[2] * rows, KEY_POS[1] * rows, KEY_POS[3] * rows
        return (
            (total.at[pl.ds(two, half)], relay.at[0], "x", 1),
            (total.at[pl.ds(two + half, half)], relay.at[1], "x", -1),
            (total.at[pl.ds(nxt + half, half)], arrive.at[0, pl.ds(half, half)], "x", 1),
            (total.at[pl.ds(prv, half)], arrive.at[1, pl.ds(0, half)], "x", -1),
            (total.at[pl.ds(nxt, half)], arrive.at[0, pl.ds(0, half)], "x", 1),
            (total.at[pl.ds(prv + half, half)], arrive.at[1, pl.ds(half, half)], "x", -1),
        )[slot]

    def message(name):
        source, target, axis, step = refs_of(name)
        return pltpu.make_async_remote_copy(
            src_ref=source,
            dst_ref=target,
            send_sem=send_sem.at[IDS[name]],
            recv_sem=recv_sem.at[IDS[name]],
            device_id=device(axis, step),
            device_id_type=MESH,
        )

    def start(*names):
        for name in names:
            message(name).start()

    def arrived(*names):
        for name in names:
            message(name).wait_recv()

    loads = [
        pltpu.make_async_copy(student_hbm, student_ref, load_sem.at[0]),
        pltpu.make_async_copy(teacher_hbm, teacher_ref, load_sem.at[1]),
    ]
    for load in loads:
        load.start()

    barrier = pltpu.get_barrier_semaphore()
    for axis in ("x", "y", "z"):
        for d in RING:
            pl.semaphore_signal(barrier, inc=1, device_id=device(axis, d), device_id_type=MESH)
    pl.semaphore_signal(barrier, inc=1, device_id=device("core", 0), device_id_type=MESH)

    for load in loads:
        load.wait()
    own_key = KEY_POS[0] * rows

    def normalise(i, carry):
        here = pl.ds(pl.multiple_of(i * 16, 16), 16)
        there = pl.ds(pl.multiple_of(own_key + i * 16, 16), 16)
        for raw, anchors, keys in ((student_ref, ua, uk), (teacher_ref, va, vk)):
            values = raw[here, :].astype(F32)
            scaling = lax.rsqrt(jnp.sum(values * values, axis=1, keepdims=True) + epsilon)
            unit = (values * scaling).astype(BF16)
            anchors[here, :] = unit
            keys[there, :] = unit
        return carry

    lax.fori_loop(0, rows // 16, normalise, 0, unroll=4)
    own_label = jnp.broadcast_to(label_ref[...].astype(F32), (8, rows))
    label_plane[0, 0, 0] = own_label
    label_line[0] = own_label
    pl.semaphore_wait(barrier, 10)

    start(*[("ly", d) for d in RING], *[("lx", d) for d in RING])
    start(*[name for name in FIRST if name not in LATER])
    start(("pu", (0, 0)), ("pv", (0, 0)))
    acc[...] = jnp.zeros_like(acc)
    total[...] = jnp.zeros_like(total)
    arrived(*[("ly", d) for d in RING])
    start(*[("lz", d) for d in RING])
    start(*LATER)

    def labels_in():
        arrived(("lp", 0), *[("lx", d) for d in RING])
        for d in range(4):
            line = label_line[d][0:1]
            key_label[key_rows(d), :] = jnp.broadcast_to(line, (rows, rows)).T
        for (dy, dz), k in SLOT.items():
            for c in range(2):
                anchor_label[:, pl.ds(k * pair + c * rows, rows)] = label_plane[c, dz, dy]

    chunk = 32
    k_rel = LOG2E / temp_student
    k_tea = LOG2E / temp_teacher

    def elementwise(k, count, base, diagonal):
        def one(i, carry):
            r = pl.ds(pl.multiple_of(base + i * chunk, chunk), chunk)
            label = key_label[r, :]
            sums = [None] * 6
            for c in range(2):
                lanes = pl.ds(c * rows, rows)
                columns = pl.ds(pl.multiple_of(k * pair + c * rows, rows), rows)
                s = raw_s[r, lanes]
                t = raw_t[r, lanes]
                b = jnp.exp2(s * k_rel - k_rel)
                w = jnp.exp2(t * k_tea - k_tea)
                same = label == jnp.broadcast_to(anchor_label[0:1, columns], label.shape)
                if diagonal and c == 0:
                    row = lax.broadcasted_iota(jnp.int32, label.shape, 0) + i * chunk
                    lane = lax.broadcasted_iota(jnp.int32, label.shape, 1)
                    other = row != lane
                    same = jnp.logical_and(same, other)
                    b = jnp.where(other, b, 0.0)
                    w = jnp.where(other, w, 0.0)
                signed_b[r, columns] = jnp.where(same, -b, b)
                w_all[r, columns] = w
                values = (b * b, b, w, w * s, jnp.where(same, s, 0.0), jnp.where(same, 1.0, 0.0))
                sums = [v if p is None else p + v for p, v in zip(sums, values)]
            for n in range(6):
                acc[n, r, :] += sums[n]
            return carry

        lax.fori_loop(0, count // chunk, one, 0, unroll=2)

    key_count = 4 * rows
    contract = (((1,), (1,)), ((), ()))

    def tile_step(k, carry):
        for n, actions in enumerate(STEPS):
            @pl.when(k == n)
            def _(n=n, actions=actions):
                for i, (name, follow, complete) in enumerate(actions):
                    if n == 0 and i == 8:
                        arrived(*[("lz", d) for d in RING])
                        start(("lp", 0))
                    arrived(name)
                    start(*follow)
                    if complete:
                        start(("p" + name[0], name[1]))
                arrived(("pu", TILES[n]), ("pv", TILES[n]))
                if n == 0:
                    labels_in()

        here = pl.ds(pl.multiple_of(k * pair, pair), pair)
        raw_s[...] = lax.dot_general(uk[...], ua[here, :], contract, preferred_element_type=F32)
        raw_t[...] = lax.dot_general(vk[...], va[here, :], contract, preferred_element_type=F32)
        elementwise(k, key_count - rows, 0, False)

        @pl.when(k == 0)
        def _():
            elementwise(k, rows, own_key, True)

        @pl.when(k > 0)
        def _():
            elementwise(k, rows, own_key, False)

        return carry

    lax.fori_loop(0, 16, tile_step, 0)

    lane = lax.broadcasted_iota(jnp.int32, (rows, rows), 1)
    for d in range(4):
        packed = jnp.zeros((rows, rows), F32)
        for n in range(6):
            packed = jnp.where(
                lane == n, jnp.sum(acc[n, key_rows(d), :], axis=1, keepdims=True), packed
            )
        part[d] = packed.T[0:8]
    start(*[("sx", d) for d in RING])
    arrived(*[("sx", d) for d in RING])
    line = lax.broadcasted_iota(jnp.int32, (8, rows), 0)

    def coefficients(e):
        sums = part[e]
        for d in RING:
            sums = sums + part_in[d - 1, (e - d) % 4]
        sup, rel, tea = sums[0:1], sums[1:2], sums[2:3]
        positives = jnp.maximum(sums[5:6], 1.0)
        coefs = (
            (1.0 / temp_sup) / sup,
            (1.0 / temp_student) / rel,
            (1.0 / temp_student) / tea,
            (1.0 / temp_sup) / positives,
        )
        if e == 0:
            contrast = (1.0 - sums[4:5] / positives) / temp_sup + jnp.log(sup)
            relation = (1.0 - sums[3:4] / tea) / temp_student + jnp.log(rel)
            mine = jnp.zeros((8, rows), F32)
            for n, value in enumerate((*coefs, contrast, relation)):
                mine = jnp.where(line == n, jnp.broadcast_to(value, (8, rows)), mine)
            coef_plane[0, 0, 0] = mine
            start(*[("s", o) for o in OTHERS])
        for n in range(4):
            key_coef[n, key_rows(e), :] = jnp.broadcast_to(coefs[n], (rows, rows)).T

    depth = 4 * rows
    chunks = 32 * rows // depth

    def fill(c, ranges, sides, out):
        size = sum(count for _, count in ranges)
        blocks = [f + i for f, count in ranges for i in range(0, count, chunk)]
        for i, first in enumerate(blocks):
            r = pl.ds(first, chunk)
            for q in range(depth // rows):
                columns = pl.ds(pl.multiple_of(c * depth + q * rows, rows), rows)
                sb = signed_b[r, columns]
                w = w_all[r, columns]
                b, a, positive = jnp.abs(sb), sb * sb, sb < 0.0
                for n, side in enumerate(sides):
                    if side == "key":
                        ca, cb, cw, cp = [key_coef[m, r, :] for m in range(4)]
                    else:
                        ca, cb, cw, cp = [
                            jnp.broadcast_to(anchor_coef[m : m + 1, columns], sb.shape)
                            for m in range(4)
                        ]
                    value = (a * ca - jnp.where(positive, cp, 0.0)) + (b * cb - w * cw)
                    there = pl.ds(n * size + i * chunk, chunk)
                    out[there, pl.ds(q * rows, rows)] = value.astype(BF16)

    def multiply(c, ranges, sides, out):
        size = sum(count for _, count in ranges)
        anchors = ua[pl.ds(pl.multiple_of(c * depth, depth), depth), :]
        made = out[pl.ds(0, size * len(sides)), :]
        product = jnp.dot(made, anchors, preferred_element_type=F32)
        if len(sides) == 2:
            product = product[0:size] + product[size : 2 * size]
        at = 0
        for first, count in ranges:
            total[pl.ds(first, count), :] += product[at : at + count]
            at += count

    def coefficients_in(c):
        for k in range(c * depth // pair, (c + 1) * depth // pair):
            dy, dz = TILES[k]
            for side in range(2):
                if (dy, dz, side) != (0, 0, 0):
                    arrived(("s", (dy, dz, side)))
                anchor_coef[:, pl.ds(k * pair + side * rows, rows)] = coef_plane[side, dz, dy]

    def second_pass(ranges, sides, staged=False):
        if staged:
            coefficients_in(0)
        fill(0, ranges, sides, gbuf0)

        def one(j, carry):
            c = 2 * j
            if staged:
                for n in range(chunks // 2):
                    @pl.when(j == n)
                    def _(n=n):
                        for piece in range(2 * n + 1, min(2 * n + 3, chunks)):
                            coefficients_in(piece)

            multiply(c, ranges, sides, gbuf0)
            fill(c + 1, ranges, sides, gbuf1)
            multiply(c + 1, ranges, sides, gbuf1)
            fill(jnp.minimum(c + 2, chunks - 1), ranges, sides, gbuf0)
            return carry

        lax.fori_loop(0, chunks // 2, one, 0)

    both = ("key", "anchor")
    coefficients(0)
    coefficients(2)
    second_pass([(0, rows)], ("key",))
    coefficients(1)
    coefficients(3)
    second_pass([(0, rows)], ("anchor",), staged=True)
    start(("r", 0), ("r", 1))
    second_pass([(KEY_POS[1] * rows + half, rows)], both)
    start(("r", 2), ("r", 3))
    second_pass([(KEY_POS[1] * rows, half), (KEY_POS[3] * rows + half, half)], both)
    arrived(("r", 0))
    total[pl.ds(KEY_POS[1] * rows, half), :] += relay[0]
    start(("r", 4))
    arrived(("r", 1))
    total[pl.ds(KEY_POS[3] * rows + half, half), :] += relay[1]
    start(("r", 5))
    losses = jnp.zeros((8, rows), F32)
    for cc in range(2):
        for zz in range(4):
            for yy in range(4):
                losses = losses + coef_plane[
                    lax.rem(cc + core, 2), lax.rem(zz + 4 - z, 4), lax.rem(yy + 4 - y, 4)
                ]
    loss_line[0] = losses
    start(*[("ox", d) for d in RING])
    second_pass([(own_key, rows)], both)

    arrived(*[("ox", d) for d in RING])
    sums = jnp.zeros((8, rows), F32)
    for xx in range(4):
        sums = sums + loss_line[lax.rem(xx + 4 - x, 4)]
    views = 128.0 * rows
    loss_ref[...] = jnp.broadcast_to(jnp.sum(sums, axis=1, keepdims=True), (8, rows)) / views

    arrived(("r", 2), ("r", 3), ("r", 4), ("r", 5))

    def finish(i, carry):
        here = pl.ds(pl.multiple_of(i * 16, 16), 16)
        there = pl.ds(pl.multiple_of(own_key + i * 16, 16), 16)
        grad_ref[here, :] = total[there, :] + arrive[0, here, :] + arrive[1, here, :]
        return carry

    lax.fori_loop(0, rows // 16, finish, 0)
    for name in NAMES:
        message(name).wait_send()


def project(
    student_hbm,
    sum_hbm,
    loss_hbm,
    grad_hbm,
    supcon_ref,
    relation_ref,
    student_ref,
    sum_ref,
    loss_ref,
    grad_ref,
    load_sem,
    store_sem,
):
    rows = student_ref.shape[0]
    piece = 32
    pieces = [pl.ds(i, piece) for i in range(0, rows, piece)]
    loads = []
    for i, here in enumerate(pieces):
        loads.append(
            (
                pltpu.make_async_copy(sum_hbm.at[here], sum_ref.at[here], load_sem.at[0, i]),
                pltpu.make_async_copy(
                    student_hbm.at[here], student_ref.at[here], load_sem.at[1, i]
                ),
            )
        )
    loss_load = pltpu.make_async_copy(loss_hbm, loss_ref, load_sem.at[2, 0])
    for pair in loads:
        for load in pair:
            load.start()
    loss_load.start()
    stores = []
    for i, here in enumerate(pieces):
        for load in loads[i]:
            load.wait()
        for r in range(0, piece, 16):
            part = pl.ds(i * piece + r, 16)
            values = student_ref[part, :].astype(F32)
            scaling = lax.rsqrt(jnp.sum(values * values, axis=1, keepdims=True) + epsilon)
            unit = values * scaling
            grad = sum_ref[part, :]
            along = jnp.sum(unit * grad, axis=1, keepdims=True)
            grad_ref[part, :] = scaling * (grad - unit * along)
        store = pltpu.make_async_copy(grad_ref.at[here], grad_hbm.at[here], store_sem.at[i])
        store.start()
        stores.append(store)
    loss_load.wait()
    supcon_ref[0, 0] = loss_ref[4, 0]
    relation_ref[0, 0] = loss_ref[5, 0]
    for store in stores:
        store.wait()


def body(student, teacher, labels):
    rows, width = student.shape
    keys, anchors = 4 * rows, 32 * rows
    vmem = pl.BlockSpec(memory_space=pltpu.VMEM)
    hbm = pl.BlockSpec(memory_space=pltpu.HBM)
    sums, losses = pl.pallas_call(
        kernel,
        out_shape=(
            jax.ShapeDtypeStruct((rows, width), F32),
            jax.ShapeDtypeStruct((8, rows), F32),
        ),
        in_specs=[hbm, hbm, vmem],
        out_specs=(vmem, vmem),
        scratch_shapes=[
            pltpu.VMEM((anchors, width), BF16),
            pltpu.VMEM((anchors, width), BF16),
            pltpu.VMEM((keys, width), BF16),
            pltpu.VMEM((keys, width), BF16),
            pltpu.VMEM((keys, 2 * rows), F32),
            pltpu.VMEM((keys, 2 * rows), F32),
            pltpu.VMEM((keys, anchors), F32),
            pltpu.VMEM((keys, anchors), F32),
            pltpu.VMEM((6, keys, rows), F32),
            pltpu.VMEM((keys, rows), F32),
            pltpu.VMEM((8, anchors), F32),
            pltpu.VMEM((2, 4, 4, 8, rows), F32),
            pltpu.VMEM((4, 8, rows), F32),
            pltpu.VMEM((4, 8, rows), F32),
            pltpu.VMEM((3, 4, 8, rows), F32),
            pltpu.VMEM((2, 4, 4, 8, rows), F32),
            pltpu.VMEM((4, keys, rows), F32),
            pltpu.VMEM((8, anchors), F32),
            pltpu.VMEM((4, 8, rows), F32),
            pltpu.VMEM((keys, 4 * rows), BF16),
            pltpu.VMEM((keys, 4 * rows), BF16),
            pltpu.VMEM((keys, width), F32),
            pltpu.VMEM((2, rows // 2, width), F32),
            pltpu.VMEM((2, rows, width), F32),
            pltpu.VMEM((rows, width), BF16),
            pltpu.VMEM((rows, width), BF16),
            pltpu.SemaphoreType.DMA((len(NAMES),)),
            pltpu.SemaphoreType.DMA((len(NAMES),)),
            pltpu.SemaphoreType.DMA((2,)),
        ],
        compiler_params=pltpu.CompilerParams(
            collective_id=0, has_side_effects=True, vmem_limit_bytes=60 * 1024 * 1024
        ),
    )(student, teacher, labels.reshape(1, rows))
    smem = pl.BlockSpec(memory_space=pltpu.SMEM)
    scalar = jax.ShapeDtypeStruct((1, 1), F32)
    grad, supcon, relation = pl.pallas_call(
        project,
        out_shape=(jax.ShapeDtypeStruct((rows, width), F32), scalar, scalar),
        in_specs=[hbm, hbm, hbm],
        out_specs=(hbm, smem, smem),
        scratch_shapes=[
            pltpu.VMEM((rows, width), BF16),
            pltpu.VMEM((rows, width), F32),
            pltpu.SMEM((8, rows), F32),
            pltpu.VMEM((rows, width), F32),
            pltpu.SemaphoreType.DMA((3, rows // 32)),
            pltpu.SemaphoreType.DMA((rows // 32,)),
        ],
    )(student, sums, losses)
    return supcon.reshape(()), relation.reshape(()), grad


def solution(mesh):
    torus = Mesh(mesh.devices.reshape(2, 2, 4, 2, 4), AXES)
    own = ("x_lo", "core", "z", "x_hi", "y")
    return jax.shard_map(
        body,
        mesh=torus,
        in_specs=(P(own, None), P(own, None), P(own)),
        out_specs=(P(), P(), P(own, None)),
        check_vma=False,
    )
```

```python
import math

import jax
import jax.numpy as jnp
from jax import lax
from jax.experimental import pallas as pl
from jax.experimental.pallas import tpu as pltpu
from jax.sharding import Mesh
from jax.sharding import PartitionSpec as P

AXES = ("x_lo", "core", "z", "x_hi", "y")
MESH = pl.DeviceIdType.MESH
F32, BF16 = jnp.float32, jnp.bfloat16

temp_sup = 0.1
temp_student = 0.2
temp_teacher = 0.05
epsilon = 1e-06
LOG2E = math.log2(math.e)

KEY_POS = {2: 0, 1: 1, 3: 2, 0: 3}
RING = (1, 2, 3)
OTHERS = [(dy, dz, c) for c in range(2) for dz in range(4) for dy in range(4)][1:]


def plane_messages():
    out = {}
    near = ((1, -1), (3, 1))

    def along(kind, axis, others):
        for d, step in near:
            for o in others:
                slot, source = ((d, o), (0, o)) if axis == "y" else ((o, d), (o, 0))
                for h in range(2):
                    out[kind, slot, h] = (source, axis, step)
        for o in others:
            for h, (d, step) in enumerate(near):
                slot, source = ((2, o), (d, o)) if axis == "y" else ((o, 2), (o, d))
                out[kind, slot, h] = (source, axis, step)

    along("u", "y", (0,))
    along("v", "z", (0,))
    along("u", "z", range(4))
    along("v", "y", range(4))
    return out


def line_messages():
    out = {}
    for kind in ("ku", "kv"):
        for d, step in ((1, -1), (3, 1)):
            for h in range(2):
                out[kind, d, h] = (0, "x", step)
        for h, (d, step) in enumerate(((1, -1), (3, 1))):
            out[kind, 2, h] = (d, "x", step)
    return out


MESSAGES = {**plane_messages(), **line_messages()}


PRIORITY = (
    62, 68, 46, 70, 12, 11, 71, 48, 31, 66, 13, 5, 35, 34, 4, 16, 19, 41,
    22, 25, 49, 54, 42, 32, 37, 6, 67, 56, 21, 40, 47, 55, 30, 8, 0, 63,
    61, 10, 24, 3, 1, 60, 18, 50, 28, 14, 2, 51, 29, 52, 64, 69, 17, 65,
    9, 53, 7, 43, 26, 20, 36, 23, 58, 38, 39, 44, 27, 45, 59, 33, 57, 15,
)


def make_schedule():
    wire, hop, tile, local = 2.82, 3.4, 1.3, 2.0
    order = dict(zip(MESSAGES, PRIORITY))
    free, arrive, waited, have = {}, {}, {}, {}

    def launch(name, when):
        _, axis, step = MESSAGES[name]
        free[axis, step] = max(free.get((axis, step), 0.0), when) + wire
        arrive[name] = free[axis, step] + hop

    def after(kind, slot, half):
        found = [
            n for n, m in MESSAGES.items() if n[0] == kind and m[0] == slot and n[2] == half
        ]
        return tuple(sorted(found, key=order.get))

    own = (("u", (0, 0)), ("v", (0, 0)), ("ku", 0), ("kv", 0))
    first = sorted((n for k in own for h in range(2) for n in after(*k, h)), key=order.get)
    for name in first:
        launch(name, 0.0)
    slots = [(dy, dz) for dz in range(4) for dy in range(4)]
    whole = {("u", (0, 0)): 0.0, ("v", (0, 0)): 0.0}
    now, tiles, steps, actions = 0.0, [], [], []
    lines = list(line_messages())

    def ready_at(slot):
        return max(whole.get((k, slot), 1e9) for k in ("u", "v")) + local

    while len(tiles) < 16:
        coming = min(((t, order[n], n) for n, t in arrive.items() if n not in waited), default=None)
        able = [s for s in slots if s not in tiles and ready_at(s) <= now]
        if not all(n in waited for n in lines):
            able = []
        if coming and (coming[0] <= now or not able):
            now = max(now, coming[0]) + 0.05
            name = coming[2]
            waited[name] = now
            follow = after(*name)
            for f in follow:
                launch(f, now)
            kind, slot, half = name
            complete = (kind, slot, 1 - half) in waited
            if complete:
                whole[kind, slot] = now
            actions.append((name, follow, complete and kind in ("u", "v")))
        elif able:
            best = min(able, key=lambda s: (ready_at(s), slots.index(s)))
            tiles.append(best)
            steps.append(tuple(actions))
            actions = []
            now += tile
        else:
            now = min(ready_at(s) for s in slots if s not in tiles) + 1e-6
    return tuple(first), tuple(steps), tuple(tiles), now


FIRST, STEPS, TILES, _ = make_schedule()
LATER = tuple(
    n
    for n in FIRST
    if MESSAGES[n][1] == "z" and n != next(m for m in FIRST if MESSAGES[m][1:] == MESSAGES[n][1:])
)
SLOT = {s: k for k, s in enumerate(TILES)}
NAMES = (
    list(MESSAGES)
    + [("pu", s) for s in TILES]
    + [("pv", s) for s in TILES]
    + [(kind, d) for kind in ("lx", "ly", "lz", "sx", "ox") for d in RING]
    + [("s", o) for o in OTHERS]
    + [("lp", 0)]
    + [("r", i) for i in range(6)]
)
IDS = {n: i for i, n in enumerate(NAMES)}


def kernel(
    student_hbm,
    teacher_hbm,
    label_ref,
    grad_ref,
    loss_ref,
    ua,
    va,
    uk,
    vk,
    raw_s,
    raw_t,
    signed_b,
    w_all,
    acc,
    key_label,
    anchor_label,
    label_plane,
    label_line,
    part,
    part_in,
    coef_plane,
    key_coef,
    anchor_coef,
    loss_line,
    gbuf0,
    gbuf1,
    total,
    relay,
    arrive,
    student_ref,
    teacher_ref,
    send_sem,
    recv_sem,
    load_sem,
):
    rows, width = student_ref.shape
    x_lo, x_hi = lax.axis_index("x_lo"), lax.axis_index("x_hi")
    core = lax.axis_index("core")
    y, z = lax.axis_index("y"), lax.axis_index("z")
    x = x_hi * 2 + x_lo
    pair = 2 * rows

    def device(axis, step):
        if axis == "core":
            return {"core": 1 - core}
        if axis == "x":
            there = lax.rem(x + step + 4, 4)
            return {"x_hi": there // 2, "x_lo": lax.rem(there, 2)}
        if axis == "plane":
            dy, dz, c = step
            there = {"y": lax.rem(y + 4 - dy, 4), "z": lax.rem(z + 4 - dz, 4)}
            return {**there, "core": 1 - core if c else core}
        place = y if axis == "y" else z
        return {axis: lax.rem(place + step + 4, 4)}

    def key_rows(d):
        return pl.ds(KEY_POS[d] * rows, rows)

    def own_rows(slot):
        return pl.ds(SLOT[slot] * pair, rows)

    half = rows // 2

    def part_of(start, h):
        return pl.ds(start + h * half, half)

    def refs_of(name):
        kind, slot = name[:2]
        if kind in ("u", "v"):
            source, axis, step = MESSAGES[name]
            buf = ua if kind == "u" else va
            here, there = SLOT[source] * pair, SLOT[slot] * pair
            return buf.at[part_of(here, name[2])], buf.at[part_of(there, name[2])], axis, step
        if kind in ("ku", "kv"):
            source, axis, step = MESSAGES[name]
            buf = uk if kind == "ku" else vk
            here, there = KEY_POS[source] * rows, KEY_POS[slot] * rows
            return buf.at[part_of(here, name[2])], buf.at[part_of(there, name[2])], axis, step
        if kind in ("pu", "pv"):
            buf = ua if kind == "pu" else va
            there = pl.ds(SLOT[slot] * pair + rows, rows)
            return buf.at[own_rows(slot)], buf.at[there], "core", 0
        if kind in ("lx", "ox"):
            buf = label_line if kind == "lx" else loss_line
            return buf.at[0], buf.at[slot], "x", -slot
        if kind == "sx":
            return part, part_in.at[slot - 1], "x", -slot
        if kind == "s":
            dy, dz, c = slot
            return coef_plane.at[0, 0, 0], coef_plane.at[c, dz, dy], "plane", slot
        if kind == "ly":
            return label_plane.at[0, 0, 0], label_plane.at[0, 0, slot], "y", -slot
        if kind == "lz":
            return label_plane.at[0, 0], label_plane.at[0, slot], "z", -slot
        if kind == "lp":
            return label_plane.at[0], label_plane.at[1], "core", 0
        two, nxt, prv = KEY_POS[2] * rows, KEY_POS[1] * rows, KEY_POS[3] * rows
        return (
            (total.at[pl.ds(two, half)], relay.at[0], "x", 1),
            (total.at[pl.ds(two + half, half)], relay.at[1], "x", -1),
            (total.at[pl.ds(nxt + half, half)], arrive.at[0, pl.ds(half, half)], "x", 1),
            (total.at[pl.ds(prv, half)], arrive.at[1, pl.ds(0, half)], "x", -1),
            (total.at[pl.ds(nxt, half)], arrive.at[0, pl.ds(0, half)], "x", 1),
            (total.at[pl.ds(prv + half, half)], arrive.at[1, pl.ds(half, half)], "x", -1),
        )[slot]

    def message(name):
        source, target, axis, step = refs_of(name)
        return pltpu.make_async_remote_copy(
            src_ref=source,
            dst_ref=target,
            send_sem=send_sem.at[IDS[name]],
            recv_sem=recv_sem.at[IDS[name]],
            device_id=device(axis, step),
            device_id_type=MESH,
        )

    def start(*names):
        for name in names:
            message(name).start()

    def arrived(*names):
        for name in names:
            message(name).wait_recv()

    loads = [
        pltpu.make_async_copy(student_hbm, student_ref, load_sem.at[0]),
        pltpu.make_async_copy(teacher_hbm, teacher_ref, load_sem.at[1]),
    ]
    for load in loads:
        load.start()

    barrier = pltpu.get_barrier_semaphore()
    for axis in ("x", "y", "z"):
        for d in RING:
            pl.semaphore_signal(barrier, inc=1, device_id=device(axis, d), device_id_type=MESH)
    pl.semaphore_signal(barrier, inc=1, device_id=device("core", 0), device_id_type=MESH)

    for load in loads:
        load.wait()
    own_key = KEY_POS[0] * rows

    def normalise(i, carry):
        here = pl.ds(pl.multiple_of(i * 16, 16), 16)
        there = pl.ds(pl.multiple_of(own_key + i * 16, 16), 16)
        for raw, anchors, keys in ((student_ref, ua, uk), (teacher_ref, va, vk)):
            values = raw[here, :].astype(F32)
            scaling = lax.rsqrt(jnp.sum(values * values, axis=1, keepdims=True) + epsilon)
            unit = (values * scaling).astype(BF16)
            anchors[here, :] = unit
            keys[there, :] = unit
        return carry

    lax.fori_loop(0, rows // 16, normalise, 0, unroll=4)
    own_label = jnp.broadcast_to(label_ref[...].astype(F32), (8, rows))
    label_plane[0, 0, 0] = own_label
    label_line[0] = own_label
    pl.semaphore_wait(barrier, 10)

    start(*[("ly", d) for d in RING], *[("lx", d) for d in RING])
    start(*[name for name in FIRST if name not in LATER])
    start(("pu", (0, 0)), ("pv", (0, 0)))
    acc[...] = jnp.zeros_like(acc)
    total[...] = jnp.zeros_like(total)
    arrived(*[("ly", d) for d in RING])
    start(*[("lz", d) for d in RING])
    start(*LATER)

    def labels_in():
        arrived(("lp", 0), *[("lx", d) for d in RING])
        for d in range(4):
            line = label_line[d][0:1]
            key_label[key_rows(d), :] = jnp.broadcast_to(line, (rows, rows)).T
        for (dy, dz), k in SLOT.items():
            for c in range(2):
                anchor_label[:, pl.ds(k * pair + c * rows, rows)] = label_plane[c, dz, dy]

    chunk = 32
    k_rel = LOG2E / temp_student
    k_tea = LOG2E / temp_teacher

    def elementwise(k, count, base, diagonal):
        def one(i, carry):
            r = pl.ds(pl.multiple_of(base + i * chunk, chunk), chunk)
            label = key_label[r, :]
            sums = [None] * 6
            for c in range(2):
                lanes = pl.ds(c * rows, rows)
                columns = pl.ds(pl.multiple_of(k * pair + c * rows, rows), rows)
                s = raw_s[r, lanes]
                t = raw_t[r, lanes]
                b = jnp.exp2(s * k_rel - k_rel)
                w = jnp.exp2(t * k_tea - k_tea)
                same = label == jnp.broadcast_to(anchor_label[0:1, columns], label.shape)
                if diagonal and c == 0:
                    row = lax.broadcasted_iota(jnp.int32, label.shape, 0) + i * chunk
                    lane = lax.broadcasted_iota(jnp.int32, label.shape, 1)
                    other = row != lane
                    same = jnp.logical_and(same, other)
                    b = jnp.where(other, b, 0.0)
                    w = jnp.where(other, w, 0.0)
                signed_b[r, columns] = jnp.where(same, -b, b)
                w_all[r, columns] = w
                values = (b * b, b, w, w * s, jnp.where(same, s, 0.0), jnp.where(same, 1.0, 0.0))
                sums = [v if p is None else p + v for p, v in zip(sums, values)]
            for n in range(6):
                acc[n, r, :] += sums[n]
            return carry

        lax.fori_loop(0, count // chunk, one, 0, unroll=2)

    key_count = 4 * rows
    contract = (((1,), (1,)), ((), ()))

    def tile_step(k, carry):
        for n, actions in enumerate(STEPS):
            @pl.when(k == n)
            def _(n=n, actions=actions):
                for i, (name, follow, complete) in enumerate(actions):
                    if n == 0 and i == 8:
                        arrived(*[("lz", d) for d in RING])
                        start(("lp", 0))
                    arrived(name)
                    start(*follow)
                    if complete:
                        start(("p" + name[0], name[1]))
                arrived(("pu", TILES[n]), ("pv", TILES[n]))
                if n == 0:
                    labels_in()

        here = pl.ds(pl.multiple_of(k * pair, pair), pair)
        raw_s[...] = lax.dot_general(uk[...], ua[here, :], contract, preferred_element_type=F32)
        raw_t[...] = lax.dot_general(vk[...], va[here, :], contract, preferred_element_type=F32)
        elementwise(k, key_count - rows, 0, False)

        @pl.when(k == 0)
        def _():
            elementwise(k, rows, own_key, True)

        @pl.when(k > 0)
        def _():
            elementwise(k, rows, own_key, False)

        return carry

    lax.fori_loop(0, 16, tile_step, 0)

    lane = lax.broadcasted_iota(jnp.int32, (rows, rows), 1)
    for d in range(4):
        packed = jnp.zeros((rows, rows), F32)
        for n in range(6):
            packed = jnp.where(
                lane == n, jnp.sum(acc[n, key_rows(d), :], axis=1, keepdims=True), packed
            )
        part[d] = packed.T[0:8]
    start(*[("sx", d) for d in RING])
    arrived(*[("sx", d) for d in RING])
    line = lax.broadcasted_iota(jnp.int32, (8, rows), 0)

    def coefficients(e):
        sums = part[e]
        for d in RING:
            sums = sums + part_in[d - 1, (e - d) % 4]
        sup, rel, tea = sums[0:1], sums[1:2], sums[2:3]
        positives = jnp.maximum(sums[5:6], 1.0)
        coefs = (
            (1.0 / temp_sup) / sup,
            (1.0 / temp_student) / rel,
            (1.0 / temp_student) / tea,
            (1.0 / temp_sup) / positives,
        )
        if e == 0:
            contrast = (1.0 - sums[4:5] / positives) / temp_sup + jnp.log(sup)
            relation = (1.0 - sums[3:4] / tea) / temp_student + jnp.log(rel)
            mine = jnp.zeros((8, rows), F32)
            for n, value in enumerate((*coefs, contrast, relation)):
                mine = jnp.where(line == n, jnp.broadcast_to(value, (8, rows)), mine)
            coef_plane[0, 0, 0] = mine
            start(*[("s", o) for o in OTHERS])
        for n in range(4):
            key_coef[n, key_rows(e), :] = jnp.broadcast_to(coefs[n], (rows, rows)).T

    depth = 4 * rows
    chunks = 32 * rows // depth

    def fill(c, ranges, sides, out):
        size = sum(count for _, count in ranges)
        blocks = [f + i for f, count in ranges for i in range(0, count, chunk)]
        for i, first in enumerate(blocks):
            r = pl.ds(first, chunk)
            for q in range(depth // rows):
                columns = pl.ds(pl.multiple_of(c * depth + q * rows, rows), rows)
                sb = signed_b[r, columns]
                w = w_all[r, columns]
                b, a, positive = jnp.abs(sb), sb * sb, sb < 0.0
                for n, side in enumerate(sides):
                    if side == "key":
                        ca, cb, cw, cp = [key_coef[m, r, :] for m in range(4)]
                    else:
                        ca, cb, cw, cp = [
                            jnp.broadcast_to(anchor_coef[m : m + 1, columns], sb.shape)
                            for m in range(4)
                        ]
                    value = (a * ca - jnp.where(positive, cp, 0.0)) + (b * cb - w * cw)
                    there = pl.ds(n * size + i * chunk, chunk)
                    out[there, pl.ds(q * rows, rows)] = value.astype(BF16)

    def multiply(c, ranges, sides, out):
        size = sum(count for _, count in ranges)
        anchors = ua[pl.ds(pl.multiple_of(c * depth, depth), depth), :]
        made = out[pl.ds(0, size * len(sides)), :]
        product = jnp.dot(made, anchors, preferred_element_type=F32)
        if len(sides) == 2:
            product = product[0:size] + product[size : 2 * size]
        at = 0
        for first, count in ranges:
            total[pl.ds(first, count), :] += product[at : at + count]
            at += count

    def coefficients_in(c):
        for k in range(c * depth // pair, (c + 1) * depth // pair):
            dy, dz = TILES[k]
            for side in range(2):
                if (dy, dz, side) != (0, 0, 0):
                    arrived(("s", (dy, dz, side)))
                anchor_coef[:, pl.ds(k * pair + side * rows, rows)] = coef_plane[side, dz, dy]

    def second_pass(ranges, sides, staged=False):
        if staged:
            coefficients_in(0)
        fill(0, ranges, sides, gbuf0)

        def one(j, carry):
            c = 2 * j
            if staged:
                for n in range(chunks // 2):
                    @pl.when(j == n)
                    def _(n=n):
                        for piece in range(2 * n + 1, min(2 * n + 3, chunks)):
                            coefficients_in(piece)

            multiply(c, ranges, sides, gbuf0)
            fill(c + 1, ranges, sides, gbuf1)
            multiply(c + 1, ranges, sides, gbuf1)
            fill(jnp.minimum(c + 2, chunks - 1), ranges, sides, gbuf0)
            return carry

        lax.fori_loop(0, chunks // 2, one, 0)

    both = ("key", "anchor")
    coefficients(0)
    coefficients(2)
    second_pass([(0, rows)], ("key",))
    coefficients(1)
    coefficients(3)
    second_pass([(0, rows)], ("anchor",), staged=True)
    start(("r", 0), ("r", 1))
    second_pass([(KEY_POS[1] * rows + half, rows)], both)
    start(("r", 2), ("r", 3))
    second_pass([(KEY_POS[1] * rows, half), (KEY_POS[3] * rows + half, half)], both)
    arrived(("r", 0))
    total[pl.ds(KEY_POS[1] * rows, half), :] += relay[0]
    start(("r", 4))
    arrived(("r", 1))
    total[pl.ds(KEY_POS[3] * rows + half, half), :] += relay[1]
    start(("r", 5))
    losses = jnp.zeros((8, rows), F32)
    for cc in range(2):
        for zz in range(4):
            for yy in range(4):
                losses = losses + coef_plane[
                    lax.rem(cc + core, 2), lax.rem(zz + 4 - z, 4), lax.rem(yy + 4 - y, 4)
                ]
    loss_line[0] = losses
    start(*[("ox", d) for d in RING])
    second_pass([(own_key, rows)], both)

    arrived(*[("ox", d) for d in RING])
    sums = jnp.zeros((8, rows), F32)
    for xx in range(4):
        sums = sums + loss_line[lax.rem(xx + 4 - x, 4)]
    views = 128.0 * rows
    loss_ref[...] = jnp.broadcast_to(jnp.sum(sums, axis=1, keepdims=True), (8, rows)) / views

    arrived(("r", 2), ("r", 3), ("r", 4), ("r", 5))

    def finish(i, carry):
        here = pl.ds(pl.multiple_of(i * 16, 16), 16)
        there = pl.ds(pl.multiple_of(own_key + i * 16, 16), 16)
        values = student_ref[here, :].astype(F32)
        scaling = lax.rsqrt(jnp.sum(values * values, axis=1, keepdims=True) + epsilon)
        unit = values * scaling
        grad = total[there, :] + arrive[0, here, :] + arrive[1, here, :]
        along = jnp.sum(unit * grad, axis=1, keepdims=True)
        grad_ref[here, :] = scaling * (grad - unit * along)
        return carry

    lax.fori_loop(0, rows // 16, finish, 0, unroll=4)
    for name in NAMES:
        message(name).wait_send()


def deliver(
    made_hbm, loss_hbm, grad_hbm, supcon_ref, relation_ref, held, loss_ref, load_sem, store_sem
):
    rows = held.shape[0]
    piece = 32
    loads, stores = [], []
    for i in range(rows // piece):
        here = pl.ds(i * piece, piece)
        loads.append(pltpu.make_async_copy(made_hbm.at[here], held.at[here], load_sem.at[i]))
        stores.append(pltpu.make_async_copy(held.at[here], grad_hbm.at[here], store_sem.at[i]))
    loss_load = pltpu.make_async_copy(loss_hbm, loss_ref, load_sem.at[rows // piece])
    for load in (*loads, loss_load):
        load.start()
    for load, store in zip(loads, stores):
        load.wait()
        store.start()
    loss_load.wait()
    supcon_ref[0, 0] = loss_ref[4, 0]
    relation_ref[0, 0] = loss_ref[5, 0]
    for store in stores:
        store.wait()


def body(student, teacher, labels):
    rows, width = student.shape
    keys, anchors = 4 * rows, 32 * rows
    vmem = pl.BlockSpec(memory_space=pltpu.VMEM)
    hbm = pl.BlockSpec(memory_space=pltpu.HBM)
    made, losses = pl.pallas_call(
        kernel,
        out_shape=(
            jax.ShapeDtypeStruct((rows, width), F32),
            jax.ShapeDtypeStruct((8, rows), F32),
        ),
        in_specs=[hbm, hbm, vmem],
        out_specs=(vmem, vmem),
        scratch_shapes=[
            pltpu.VMEM((anchors, width), BF16),
            pltpu.VMEM((anchors, width), BF16),
            pltpu.VMEM((keys, width), BF16),
            pltpu.VMEM((keys, width), BF16),
            pltpu.VMEM((keys, 2 * rows), F32),
            pltpu.VMEM((keys, 2 * rows), F32),
            pltpu.VMEM((keys, anchors), F32),
            pltpu.VMEM((keys, anchors), F32),
            pltpu.VMEM((6, keys, rows), F32),
            pltpu.VMEM((keys, rows), F32),
            pltpu.VMEM((8, anchors), F32),
            pltpu.VMEM((2, 4, 4, 8, rows), F32),
            pltpu.VMEM((4, 8, rows), F32),
            pltpu.VMEM((4, 8, rows), F32),
            pltpu.VMEM((3, 4, 8, rows), F32),
            pltpu.VMEM((2, 4, 4, 8, rows), F32),
            pltpu.VMEM((4, keys, rows), F32),
            pltpu.VMEM((8, anchors), F32),
            pltpu.VMEM((4, 8, rows), F32),
            pltpu.VMEM((keys, 4 * rows), BF16),
            pltpu.VMEM((keys, 4 * rows), BF16),
            pltpu.VMEM((keys, width), F32),
            pltpu.VMEM((2, rows // 2, width), F32),
            pltpu.VMEM((2, rows, width), F32),
            pltpu.VMEM((rows, width), BF16),
            pltpu.VMEM((rows, width), BF16),
            pltpu.SemaphoreType.DMA((len(NAMES),)),
            pltpu.SemaphoreType.DMA((len(NAMES),)),
            pltpu.SemaphoreType.DMA((2,)),
        ],
        compiler_params=pltpu.CompilerParams(
            collective_id=0, has_side_effects=True, vmem_limit_bytes=60 * 1024 * 1024
        ),
    )(student, teacher, labels.reshape(1, rows))
    smem = pl.BlockSpec(memory_space=pltpu.SMEM)
    scalar = jax.ShapeDtypeStruct((1, 1), F32)
    grad, supcon, relation = pl.pallas_call(
        deliver,
        out_shape=(jax.ShapeDtypeStruct((rows, width), F32), scalar, scalar),
        in_specs=[hbm, hbm],
        out_specs=(hbm, smem, smem),
        scratch_shapes=[
            pltpu.VMEM((rows, width), F32),
            pltpu.SMEM((8, rows), F32),
            pltpu.SemaphoreType.DMA((rows // 32 + 1,)),
            pltpu.SemaphoreType.DMA((rows // 32,)),
        ],
    )(made, losses)
    return supcon.reshape(()), relation.reshape(()), grad


def solution(mesh):
    torus = Mesh(mesh.devices.reshape(2, 2, 4, 2, 4), AXES)
    own = ("x_lo", "core", "z", "x_hi", "y")
    return jax.shard_map(
        body,
        mesh=torus,
        in_specs=(P(own, None), P(own, None), P(own)),
        out_specs=(P(), P(), P(own, None)),
        check_vma=False,
    )
```
